32 devices in a mesh: leaf: 8 (over z, y), hand: 4 (over x, core).
Axes of the slice: x: 2, y: 2, z: 4, core: 2. Of those that a mesh axis runs over, the one named last changes fastest.
Arguments:
- opp_range: float32 [1024], P('hand'), may hold values from 0.1 to 1
- br_range: float32 [1024], P('hand'), may hold values from 0.001 to 1
- up_weight: bfloat16 [4, 256, 1024], P(None, 'leaf', 'hand'), may hold values from 0.29882812 to 1
- up_parent: int32 [3, 256], replicated, may hold values from 0 to 255
- board_cards: int32 [768, 5], P('leaf'), may hold values from 0 to 51, as said below
- hand_rank: int32 [768, 1024], P('leaf'), may hold values from 0 to 7461
- root_parent: int32 [768], P('leaf'), may hold values from 0 to 255
- br_actions: int32 [768], P('leaf'), may hold values from 1 to 8
- opp_actions: int32 [768, 8], P('leaf'), may hold values from 1 to 8
- leaf_kind: int32 [768, 8, 8], P('leaf'), may hold values from 0 to 1
- leaf_stake: int32 [768, 8, 8], P('leaf'), may hold values from 1 to 400
- opp_weight: bfloat16 [768, 8, 8, 1024], P('leaf', None, None, 'hand'), may hold values from 0.049804688 to 1
Outputs:
- level_values: float32 [4, 256, 1024], P(None, 'leaf', 'hand')
- root_value: float32 [1024], P('hand')
- best_value: float32 [], replicated
The draws below stay inside these ranges and needn't reach their ends.
Inputs may be any that keep to these rules, and one draw needn't show every extreme that they name: `board_cards`: five different cards for each subtree.
All inputs are finite; a program needn't handle non-finite values.
Results may differ from the reference program's by a relative error of at most 0.0003.
Values may be sent and summed in bfloat16 or wider, within the bound.
A program may use at most 128 MiB of HBM per device.

```python
import math
import jax
import jax.numpy as jnp
import numpy as np
from jax import lax

HANDS = 1024
ACT = 8
UP = 4
UNODES = 256
SUBTREES = 768


def pick_cards(subkey):
    return jax.random.permutation(subkey, 52)[:5]


def draw_board_cards(key, part):
    subkeys = jax.random.split(jax.random.fold_in(key, 17), SUBTREES)
    return jax.vmap(pick_cards)(subkeys).astype(jnp.int32)


def set_ends(values, stream_key, least, high):
    shape = values.shape
    index_at = [jax.random.randint(jax.random.fold_in(stream_key, axis), (), 0, shape[axis]) for axis in range(len(shape))]
    values = values.at[tuple(index_at)].set(least)
    longest = shape.index(max(shape))
    index_at[longest] = (index_at[longest] + 1) % shape[longest]
    return values.at[tuple(index_at)].set(high)


def block_scale(key, extent, pieces, least, high):
    level, own = 1.0, jax.random.fold_in(key, 6)
    for dim, parts in pieces:
        steps = jnp.exp(jax.random.uniform(jax.random.fold_in(own, dim), (parts,), jnp.float32, least / len(pieces), high / len(pieces)))
        level = level * jnp.repeat(steps, extent[dim] // parts).reshape([-1 if axis == dim else 1 for axis in range(len(extent))])
    return level


def setup_inputs(seed: int = 0) -> dict:
    arg_keys = jax.random.split(jax.random.key(seed), 13)
    return {
        "opp_range": jnp.clip(jnp.exp(math.log(1.0) - 2.3025851 * jax.random.uniform(arg_keys[0], (HANDS,), jnp.float32) ** block_scale(arg_keys[0], (HANDS,), ((0, 4),), -0.2, 0.2)), 0.1, 1.0),
        "br_range": jnp.clip(jnp.exp(math.log(1.0) - 6.9077552 * jax.random.uniform(arg_keys[1], (HANDS,), jnp.float32) ** block_scale(arg_keys[1], (HANDS,), ((0, 4),), -0.2, 0.2)), 0.001, 1.0),
        "up_weight": jnp.clip(jnp.exp(math.log(1.0) - 1.2078867 * jax.random.uniform(arg_keys[2], (UP, UNODES, HANDS), jnp.float32) ** block_scale(arg_keys[2], (UP, UNODES, HANDS), ((1, 8), (2, 4)), -0.2, 0.2)), 0.29882812, 1.0).astype(jnp.bfloat16),
        "up_parent": set_ends(jax.random.randint(arg_keys[3], (UP - 1, UNODES), 0, UNODES), jax.random.fold_in(arg_keys[3], 1), 0, UNODES - 1).astype(jnp.int32),
        "board_cards": draw_board_cards(jax.random.fold_in(arg_keys[12], 71), 0),
        "hand_rank": set_ends(jax.random.randint(arg_keys[5], (SUBTREES, HANDS), 0, 7462), jax.random.fold_in(arg_keys[5], 1), 0, 7461).astype(jnp.int32),
        "root_parent": set_ends(jax.random.randint(arg_keys[6], (SUBTREES,), 0, UNODES), jax.random.fold_in(arg_keys[6], 1), 0, UNODES - 1).astype(jnp.int32),
        "br_actions": set_ends(jax.random.randint(arg_keys[7], (SUBTREES,), 1, ACT + 1), jax.random.fold_in(arg_keys[7], 1), 1, ACT).astype(jnp.int32),
        "opp_actions": set_ends(jax.random.randint(arg_keys[8], (SUBTREES, ACT), 1, ACT + 1), jax.random.fold_in(arg_keys[8], 1), 1, ACT).astype(jnp.int32),
        "leaf_kind": set_ends(jax.random.randint(arg_keys[9], (SUBTREES, ACT, ACT), 0, 2), jax.random.fold_in(arg_keys[9], 1), 0, 1).astype(jnp.int32),
        "leaf_stake": set_ends(jax.random.randint(arg_keys[10], (SUBTREES, ACT, ACT), 1, 401), jax.random.fold_in(arg_keys[10], 1), 1, 400).astype(jnp.int32),
        "opp_weight": jnp.clip(jnp.exp(math.log(1.0) - 2.9996462 * jax.random.uniform(arg_keys[11], (SUBTREES, ACT, ACT, HANDS), jnp.float32) ** block_scale(arg_keys[11], (SUBTREES, ACT, ACT, HANDS), ((0, 8), (3, 4)), -0.2, 0.2)), 0.049804688, 1.0).astype(jnp.bfloat16),
    }


PAYOFF_UNIT = 1.0 / 4096.0


def hand_cards(number):
    low_list = []
    high_list = []
    for low_card in range(52):
        for high_card in range(low_card + 1, 52):
            low_list.append(low_card)
            high_list.append(high_card)
    chosen = (np.arange(number) * 1326) // number
    return np.array(low_list, np.int32)[chosen], np.array(high_list, np.int32)[chosen]


def no_shared(low_rows, high_rows, low_cols, high_cols):
    apart_mask = (low_rows[:, None] != low_cols[None, :]) & (low_rows[:, None] != high_cols[None, :])
    apart_mask = apart_mask & (high_rows[:, None] != low_cols[None, :]) & (high_rows[:, None] != high_cols[None, :])
    return apart_mask.astype(jnp.float32)


def board_compat(board_cards, low_cols, high_cols):
    hits = (board_cards[:, :, None] == low_cols[None, None, :]) | (board_cards[:, :, None] == high_cols[None, None, :])
    return 1.0 - jnp.any(hits, axis=1).astype(jnp.float32)


def board_values(packed, noshare):
    root_row, compat_row, rank_row, opp_count, br_count, kind_rows, stake_rows, weight_rows = packed
    legal_mask = (jnp.arange(ACT)[None, :] < opp_count[:, None]).astype(jnp.float32)
    weighted = weight_rows.astype(jnp.float32) * legal_mask[:, :, None]
    probability = weighted / jnp.sum(weighted, axis=1, keepdims=True)
    leaf_reach = (root_row[None, None, :] * probability).astype(jnp.bfloat16).reshape(ACT * ACT, HANDS)
    reach_wide = leaf_reach.astype(jnp.float32)
    order_sign = jnp.sign(rank_row[None, :] - rank_row[:, None]).astype(jnp.float32) * noshare
    showdown = jnp.dot(reach_wide, order_sign, precision=lax.Precision.HIGHEST)
    folded = jnp.dot(reach_wide, noshare, precision=lax.Precision.HIGHEST)
    stake_scaled = stake_rows.reshape(-1).astype(jnp.float32) * PAYOFF_UNIT
    payoff = jnp.where(kind_rows.reshape(-1)[:, None] == 1, showdown, folded) * stake_scaled[:, None] * compat_row[None, :]
    per_node = jnp.sum(payoff.reshape(ACT, ACT, HANDS), axis=1)
    allowed = jnp.arange(ACT)[:, None] < br_count
    return jnp.max(jnp.where(allowed, per_node, -1e30), axis=0)


def reference(opp_range, br_range, up_weight, up_parent, board_cards, hand_rank, root_parent, br_actions, opp_actions, leaf_kind, leaf_stake, opp_weight):
    low_np, high_np = hand_cards(HANDS)
    low_all = jnp.asarray(low_np)
    high_all = jnp.asarray(high_np)
    compat = board_compat(board_cards, low_all, high_all)
    noshare = no_shared(low_all, high_all, low_all, high_all)
    reach_now = opp_range[None, :] * up_weight[0].astype(jnp.float32)
    for level_id in range(1, UP):
        reach_now = jnp.take(reach_now, up_parent[level_id - 1], axis=0) * up_weight[level_id].astype(jnp.float32)
    root_reach = jnp.take(reach_now, root_parent, axis=0) * compat

    def one_board(packed):
        return board_values(packed, noshare)

    sub_value = lax.map(one_board, (root_reach, compat, hand_rank, opp_actions, br_actions, leaf_kind, leaf_stake, opp_weight))
    level_sum = jax.ops.segment_sum(sub_value, root_parent, num_segments=UNODES)
    level_list = [level_sum]
    for level_id in range(UP - 1, 0, -1):
        level_sum = jax.ops.segment_sum(level_sum, up_parent[level_id - 1], num_segments=UNODES)
        level_list.insert(0, level_sum)
    level_values = jnp.stack(level_list)
    root_value = jnp.sum(level_values[0], axis=0) / UNODES
    best_value = jnp.sum(br_range * root_value) / jnp.sum(br_range)
    return level_values, root_value, best_value
```

```python
import functools

import jax
import jax.numpy as jnp
import numpy as np
from jax import lax
from jax.experimental import pallas as pl
from jax.experimental.pallas import tpu as pltpu
from jax.sharding import PartitionSpec as P

PAYOFF_UNIT = 1.0 / 4096.0
VMEM_LIMIT = 60 * 1024 * 1024
F32 = jnp.float32
BF16 = jnp.bfloat16


def hand_cards(number):
    low_list = []
    high_list = []
    for low_card in range(52):
        for high_card in range(low_card + 1, 52):
            low_list.append(low_card)
            high_list.append(high_card)
    chosen = np.arange(number) * 1326 // number
    cards = np.zeros((8, number), np.float32)
    cards[0] = np.array(low_list)[chosen]
    cards[1] = np.array(high_list)[chosen]
    cards[2] = np.exp2(np.arange(number) * 0.6180339887498949 % 1.0)
    cards[3] = 1.0 / cards[2]
    return cards


def vmem():
    return pl.BlockSpec(memory_space=pltpu.VMEM)


def hbm():
    return pl.BlockSpec(memory_space=pl.ANY)


def greet(axes_sizes):
    barrier = pltpu.get_barrier_semaphore()
    count = 0
    for axis, size in axes_sizes:
        me = lax.axis_index(axis)
        for dist in range(1, size):
            pl.semaphore_signal(
                barrier,
                inc=1,
                device_id={axis: lax.rem(me + dist, size)},
                device_id_type=pl.DeviceIdType.MESH,
            )
            count += 1
    pl.semaphore_wait(barrier, count)


def flip(index, mask):
    out = index
    bit = 1
    while bit <= mask:
        if mask & bit:
            out = out + bit - 2 * bit * lax.rem(index // bit, 2)
        bit *= 2
    return out


def peers_of(me, size):
    if size & (size - 1):
        return [lax.rem(me + dist, size) for dist in range(1, size)]
    far = [mask for mask in range(1, size) if mask >= size // 2]
    near = [mask for mask in range(1, size) if mask < size // 2]
    return [flip(me, mask) for mask in far + near]


def push(axis, size, source, target, sem):
    me = lax.axis_index(axis)
    copies = []
    for k in range(size - 1):
        peer = lax.rem(me + k + 1, size)
        copies.append(push_one(axis, peer, source(peer), target, sem, k))
    return copies


def push_one(axis, peer, source, target, sem, k):
    send_sem, recv_sem = sem
    copy = pltpu.make_async_remote_copy(
        src_ref=source,
        dst_ref=target,
        send_sem=send_sem.at[k],
        recv_sem=recv_sem.at[k],
        device_id={axis: peer},
        device_id_type=pl.DeviceIdType.MESH,
    )
    copy.start()
    return copy


def sems(*shape):
    return pltpu.SemaphoreType.DMA(shape[:-1] + (max(shape[-1] - 1, 1),))


def columns_of(ref, pad_ref):
    lines, count = ref.shape
    pad_ref[...] = jnp.zeros(pad_ref.shape, F32)
    pad_ref[0:lines, 0:count] = ref[...].astype(F32)
    return pad_ref[...].T


def kernel(
    leafs, hands, levels, actions,
    upper_ref, parent_ref, root_ref, board_ref, range_ref, br_ref, cards_ref, opp_ref, kind_ref, stake_ref,
    actions_ref, rank_ref, weight_ref,
    level_out, root_out, best_out,
    every, weights, ranks_in, ratio, ratio_in, reach, reach_in, anc, anc_all, br_all,
    pad, board_columns, stake_lines, stake_rows, apart_ref, against_ref, scaled,
    ready, mine, values_all, tally, tally_leaf, tally_all,
    up_s, up_r, anc_s, anc_r, ratio_s, ratio_r, reach_s, reach_r, br_s, br_r,
    hand_s, hand_r, leaf_s, leaf_r, tally_s, tally_r, total_s, total_r, load_sem, own_sem,
):
    leaf = lax.axis_index("leaf")
    hand = lax.axis_index("hand")
    count = ratio.shape[1] // (2 * actions)
    width = weights.shape[3]
    boards = hands * count
    chunks = count // 8
    all_hands = hands * width
    span = actions * actions
    both = 2 * actions
    nodes_dev = upper_ref.shape[1]
    nodes = leafs * nodes_dev
    partners = peers_of(hand, hands)

    def load(part, chunk, slot):
        first = pl.multiple_of(part * count + chunk * 8, 8)
        return pltpu.make_async_copy(
            weight_ref.at[pl.ds(first, 8)], weights.at[part, pl.ds(chunk * 8, 8)], load_sem.at[slot, chunk]
        )

    parts = partners + [hand]
    for chunk in range(chunks):
        for k, part in enumerate(parts):
            load(part, chunk, k).start()
    own_upper = pltpu.make_async_copy(upper_ref, every.at[leaf], own_sem.at[0])
    own_upper.start()
    own_ranks = pltpu.make_async_copy(
        rank_ref.at[pl.ds(pl.multiple_of(hand * count, 8), count)], ranks_in, own_sem.at[1]
    )
    own_ranks.start()
    greet((("leaf", leafs), ("hand", hands)))
    up_copies = push("leaf", leafs, lambda peer: upper_ref, every.at[leaf], (up_s, up_r))

    stake_lines[...] = jnp.zeros(stake_lines.shape, F32)
    reply_ids = lax.broadcasted_iota(jnp.int32, (actions, boards), 0)
    for a in range(actions):
        lines = slice(a * actions, (a + 1) * actions)
        stake = stake_ref[lines, :]
        signed = jnp.where(kind_ref[lines, :] == 1, stake, -stake)
        legal = reply_ids < opp_ref[a : a + 1, :]
        stake_lines[lines, 0:boards] = jnp.where(legal, signed, 0).astype(F32)
    stake_rows[...] = stake_lines[...].T

    diagonal = lax.broadcasted_iota(jnp.int32, (actions, span), 0) == (
        lax.broadcasted_iota(jnp.int32, (actions, span), 1) // actions
    )
    own_lanes = pl.ds(pl.multiple_of(hand * width, width), width)
    spread = cards_ref[2:3, own_lanes]

    def fold(part, chunk, target):
        lines = stake_rows[pl.ds(pl.multiple_of(part * count + chunk * 8, 8), 8), :]
        for i in range(8):
            stake = jnp.broadcast_to(lines[i : i + 1, :], (actions, span))
            stake = jnp.where(diagonal, stake, 0.0)
            legal = jnp.where(stake != 0.0, 1.0, 0.0)
            shown = jnp.maximum(stake, 0.0)
            folds = jnp.maximum(-stake, 0.0)
            shown_hi = jnp.floor(shown * 0.5) * 2.0
            fold_hi = jnp.floor(folds * 0.5) * 2.0
            rows = jnp.concatenate([legal, shown_hi, shown - shown_hi, fold_hi, folds - fold_hi], axis=0)
            sums = jnp.dot(rows.astype(BF16), weights[part, chunk * 8 + i], preferred_element_type=F32)
            piece = [sums[j * actions : (j + 1) * actions] for j in range(5)]
            scale = spread / piece[0]
            pair = jnp.concatenate(
                [(piece[1] + piece[2]) * scale, (piece[3] + piece[4]) * scale], axis=0
            )
            place = (chunk * 8 + i) * both
            target[part, place : place + both, :] = pair.astype(BF16)

    ratio_copies = []
    for chunk in range(chunks):
        block = pl.ds(chunk * 8 * both, 8 * both)
        for k, part in enumerate(partners):
            load(part, chunk, k).wait()
            fold(part, chunk, ratio)
            ratio_copies.append(
                push_one(
                    "hand", part, ratio.at[part, block], ratio_in.at[hand, block],
                    (ratio_s.at[chunk], ratio_r.at[chunk]), k,
                )
            )
    br_copies = push("hand", hands, lambda peer: br_ref, br_all.at[hand], (br_s, br_r))
    br_all[hand] = br_ref[...]

    node_column = lax.broadcasted_iota(jnp.int32, (nodes, boards), 0)
    pad[...] = jnp.zeros(pad.shape, F32)
    line = root_ref[...]
    pad[levels - 1 : levels, 0:boards] = line.astype(F32)
    for level in range(levels - 2, -1, -1):
        parents = jnp.broadcast_to(parent_ref[level : level + 1, :], (8, nodes)).astype(F32)
        column = parents.T[:, 0:1]
        line_f = jnp.sum(jnp.where(node_column == line, column, 0.0), axis=0, keepdims=True)
        pad[level : level + 1, 0:boards] = line_f
        line = line_f.astype(jnp.int32)
    anc_float = pad[...].T
    anc_columns = anc_float.astype(jnp.int32)
    lane = lax.broadcasted_iota(jnp.int32, (boards, boards), 1)
    held = (lane % (hands * 8)) // 8 * count + lane // (hands * 8) * 8 + lane % 8
    moved = lax.broadcasted_iota(jnp.int32, (boards, boards), 0) == held
    anc[...] = jnp.zeros(anc.shape, F32)
    for level in range(levels):
        anc[level : level + 1, 0:boards] = jnp.sum(
            jnp.where(moved, anc_float[0:boards, level : level + 1], 0.0), axis=0, keepdims=True
        )
    anc_copies = push("leaf", leafs, lambda peer: anc, anc_all.at[leaf], (anc_s, anc_r))
    anc_all[leaf] = anc[...]

    low = cards_ref[0:1, :]
    high = cards_ref[1:2, :]
    card_columns = cards_ref[...].T
    for part in range(hands):
        rows = slice(part * width, (part + 1) * width)
        low_col = card_columns[rows, 0:1]
        high_col = card_columns[rows, 1:2]
        hit = (low_col == low) | (low_col == high) | (high_col == low) | (high_col == high)
        apart_ref[rows, :] = jnp.where(hit, 0.0, 1.0).astype(BF16)
        against_ref[rows, :] = jnp.where(hit, 0.0, -1.0).astype(BF16)

    for chunk in range(chunks):
        load(hand, chunk, hands - 1).wait()
        fold(hand, chunk, ratio_in)

    own_low = cards_ref[0:1, own_lanes]
    own_high = cards_ref[1:2, own_lanes]
    board_columns[...] = columns_of(board_ref, pad)
    free = jnp.ones((boards, width), F32)
    for card in range(5):
        column = board_columns[0:boards, card : card + 1]
        free = jnp.where((column == own_low) | (column == own_high), 0.0, free)
    free = free * cards_ref[3:4, own_lanes]

    own_ranks.wait()
    ranks = ((ranks_in[...] % 128) + 128).astype(F32)
    octave = ranks_in[...] // 128
    for bit in (1, 2, 4, 8, 16, 32):
        ranks = ranks * jnp.where(octave // bit % 2 == 1, float(2**bit), 1.0)
    scaled[...] = ranks

    own_upper.wait()
    for copy in up_copies:
        copy.wait()
    node_ids = lax.broadcasted_iota(jnp.int32, (boards, nodes), 1)
    total = jnp.broadcast_to(range_ref[...], (boards, width))
    for level in range(levels):
        pick = jnp.where(anc_columns[0:boards, level : level + 1] == node_ids, 1.0, 0.0).astype(BF16)
        table = every[:, level].reshape(nodes, width)
        total = total * jnp.dot(pick, table, preferred_element_type=F32)
    total = total * free
    for part in range(hands):
        reach[part] = total[part * count : (part + 1) * count].astype(BF16)
    reach_copies = []
    for k, part in enumerate(partners):
        reach_copies.append(
            push_one("hand", part, reach.at[part], reach_in.at[hand], (reach_s, reach_r), k)
        )
    reach_in[hand] = reach[hand]
    action_ids = lax.broadcasted_iota(jnp.int32, (actions, 1), 0)
    for copy in br_copies:
        copy.wait()
    br_row = jnp.concatenate([br_all[part] for part in range(hands)], axis=1)
    for copy in reach_copies:
        copy.wait()

    def values(chunk, midway):
        first = pl.multiple_of(hand * count + chunk * 8, 8)
        cards_on = board_columns[pl.ds(first, 8), :]
        open_hands = jnp.ones((8, all_hands), F32)
        for card in range(5):
            column = cards_on[:, card : card + 1]
            open_hands = jnp.where((column == low) | (column == high), 0.0, open_hands)
        rank_rows = scaled[chunk * 8 : chunk * 8 + 8, :]
        rank_columns = rank_rows.T.astype(BF16)
        rank_rows = rank_rows.astype(BF16)
        lines = []
        folded = jnp.zeros((8 * both, all_hands), F32)
        for part in range(hands):
            pieces = []
            reach_rows = reach_in[part, chunk * 8 : chunk * 8 + 8, :].astype(F32)
            for i in range(8):
                b = chunk * 8 + i
                row = ratio_in[part, b * both : (b + 1) * both, :].astype(F32)
                pieces.append((row * reach_rows[i : i + 1, :]).astype(BF16))
            lines.append(pieces)
            folded = folded + jnp.dot(
                jnp.concatenate(pieces, axis=0),
                apart_ref[part * width : (part + 1) * width, :],
                preferred_element_type=F32,
            )
        best_rows = []
        for i in range(8):
            if i == 4:
                midway()
            shown = jnp.zeros((both, all_hands), F32)
            for part in range(hands):
                rows = slice(part * width, (part + 1) * width)
                order = rank_rows[i : i + 1, :] - rank_columns[rows, i : i + 1]
                order = jnp.minimum(jnp.maximum(order, against_ref[rows, :]), apart_ref[rows, :])
                shown = shown + jnp.dot(lines[part][i], order, preferred_element_type=F32)
            per_node = shown[0:actions] + folded[i * both + actions : (i + 1) * both]
            allowed = action_ids < actions_ref[first + i]
            best_rows.append(jnp.max(jnp.where(allowed, per_node, -1e30), axis=0, keepdims=True))
        best = jnp.concatenate(best_rows, axis=0) * (open_hands * PAYOFF_UNIT)
        for part in range(hands):
            ready[chunk, part] = best[:, part * width : (part + 1) * width]
        return jnp.sum(best * br_row, axis=1, keepdims=True)

    def to_hands(chunk):
        copies = [
            push_one(
                "hand", part, ready.at[chunk, part], mine.at[chunk, hand],
                (hand_s.at[chunk], hand_r.at[chunk]), k,
            )
            for k, part in enumerate(partners)
        ]
        mine[chunk, hand] = ready[chunk, hand]
        return copies

    def to_leafs(chunk, copies):
        for copy in copies:
            copy.wait()
        copies = push(
            "leaf", leafs, lambda peer: mine.at[chunk], values_all.at[chunk, leaf],
            (leaf_s.at[chunk], leaf_r.at[chunk]),
        )
        values_all[chunk, leaf] = mine[chunk]
        return copies

    leaf_copies = []
    hand_copies = []

    def relay(chunk):
        if chunk >= 0:
            leaf_copies.append(to_leafs(chunk, hand_copies))

    weighed = jnp.zeros((8, 1), F32)
    for chunk in range(chunks):
        for copy in ratio_copies[chunk * (hands - 1) : (chunk + 1) * (hands - 1)]:
            copy.wait()
        weighed = weighed + values(chunk, functools.partial(relay, chunk - 1))
        if chunk == chunks - 1:
            share = jnp.broadcast_to(jnp.sum(weighed, axis=0, keepdims=True), (1, 128))
            tally[hand, 0:1] = share
            tally_copies = [
                push_one(
                    "hand", part, tally.at[hand, pl.ds(0, 1)], tally.at[hand, pl.ds(0, 1)], (tally_s, tally_r), k
                )
                for k, part in enumerate(partners)
            ]
        hand_copies = to_hands(chunk)
    leaf_copies.append(to_leafs(chunks - 1, hand_copies))
    for copy in tally_copies:
        copy.wait()
    tally_leaf[0:1, :] = sum(tally[part, 0:1] for part in range(hands))
    total_copies = push(
        "leaf", leafs, lambda peer: tally_leaf.at[pl.ds(0, 1)], tally_all.at[leaf, pl.ds(0, 1)], (total_s, total_r)
    )
    tally_all[leaf, 0:1] = tally_leaf[0:1, :]

    for copy in anc_copies:
        copy.wait()
    lines_dev = levels * nodes_dev
    block = hands * 8
    node_rows = leaf * nodes_dev + lax.broadcasted_iota(jnp.int32, (nodes_dev, block), 0)
    node_rows = node_rows.astype(F32)

    def add_chunk(chunk, sums):
        def add_leaf(source, sums):
            part = values_all[chunk, source].reshape(block, width)
            coarse = part.astype(BF16)
            fine = (part - coarse.astype(F32)).astype(BF16)
            lines = anc_all[source][:, chunk * block : (chunk + 1) * block]
            pick = [jnp.where(lines[k : k + 1, :] == node_rows, 1.0, 0.0) for k in range(levels)]
            pick = jnp.concatenate(pick + [jnp.ones((8, block), F32)], axis=0).astype(BF16)
            sums = sums + jnp.dot(pick, coarse, preferred_element_type=F32)
            return sums + jnp.dot(pick, fine, preferred_element_type=F32)

        for source in range(leafs):
            sums = add_leaf(source, sums)
        return sums

    sums = jnp.zeros((lines_dev + 8, width), F32)
    for chunk in range(chunks):
        for copy in leaf_copies[chunk]:
            copy.wait()
        sums = add_chunk(chunk, sums)
    root_out[...] = sums[lines_dev : lines_dev + 1] / nodes
    for k in range(levels):
        level_out[k] = sums[k * nodes_dev : (k + 1) * nodes_dev]
    for copy in total_copies:
        copy.wait()
    whole = sum(tally_all[source, 0:1] for source in range(leafs)) / nodes
    best_out[...] = whole[:, 0:1] / jnp.sum(br_row, axis=1, keepdims=True)


def evaluate(
    upper, parents, roots, boards, opp_range, br_range, cards, opp_actions, kinds, stakes,
    br_actions, ranks, weights, leafs, hands, actions,
):
    levels, nodes_dev, width = upper.shape
    boards_dev, span, _ = weights.shape
    count = boards_dev // hands
    chunks = count // 8
    both = 2 * actions
    all_hands = ranks.shape[1]
    lanes = -(-boards_dev // 128) * 128
    return pl.pallas_call(
        functools.partial(kernel, leafs, hands, levels, actions),
        out_shape=(
            jax.ShapeDtypeStruct((levels, nodes_dev, width), F32),
            jax.ShapeDtypeStruct((1, width), F32),
            jax.ShapeDtypeStruct((1, 1), F32),
        ),
        in_specs=[vmem()] * 10 + [pl.BlockSpec(memory_space=pltpu.SMEM), hbm(), hbm()],
        out_specs=(vmem(), vmem(), vmem()),
        scratch_shapes=[
            pltpu.VMEM((leafs, levels, nodes_dev, width), BF16),
            pltpu.VMEM((hands, count, span, width), BF16),
            pltpu.VMEM((count, all_hands), jnp.int32),
            pltpu.VMEM((hands, count * both, width), BF16),
            pltpu.VMEM((hands, count * both, width), BF16),
            pltpu.VMEM((hands, count, width), BF16),
            pltpu.VMEM((hands, count, width), BF16),
            pltpu.VMEM((8, lanes), F32),
            pltpu.VMEM((leafs, 8, lanes), F32),
            pltpu.VMEM((hands, 1, width), F32),
            pltpu.VMEM((8, lanes), F32),
            pltpu.VMEM((lanes, 8), F32),
            pltpu.VMEM((span, lanes), F32),
            pltpu.VMEM((lanes, span), F32),
            pltpu.VMEM((all_hands, all_hands), BF16),
            pltpu.VMEM((all_hands, all_hands), BF16),
            pltpu.VMEM((count, all_hands), F32),
            pltpu.VMEM((chunks, hands, 8, width), F32),
            pltpu.VMEM((chunks, hands, 8, width), F32),
            pltpu.VMEM((chunks, leafs, hands, 8, width), F32),
            pltpu.VMEM((hands, 8, 128), F32),
            pltpu.VMEM((8, 128), F32),
            pltpu.VMEM((leafs, 8, 128), F32),
            sems(leafs), sems(leafs), sems(leafs), sems(leafs),
            sems(chunks, hands), sems(chunks, hands), sems(hands), sems(hands), sems(hands), sems(hands),
            sems(chunks, hands), sems(chunks, hands), sems(chunks, leafs), sems(chunks, leafs),
            sems(hands), sems(hands), sems(leafs), sems(leafs),
            pltpu.SemaphoreType.DMA((hands, chunks)),
            pltpu.SemaphoreType.DMA((2,)),
        ],
        compiler_params=pltpu.CompilerParams(
            collective_id=0, has_side_effects=True, vmem_limit_bytes=VMEM_LIMIT
        ),
        name="evaluate",
    )(
        upper, parents, roots, boards, opp_range, br_range, cards, opp_actions, kinds, stakes,
        br_actions, ranks, weights,
    )


def local(
    opp_range,
    br_range,
    up_weight,
    up_parent,
    board_cards,
    hand_rank,
    root_parent,
    br_actions,
    opp_actions,
    leaf_kind,
    leaf_stake,
    opp_weight,
):
    hands_dev = up_weight.shape[2]
    boards_dev, hands_all = hand_rank.shape
    actions = opp_actions.shape[1]
    span = actions * actions
    leafs = lax.axis_size("leaf")
    hands = lax.axis_size("hand")
    cards = jnp.asarray(hand_cards(hands_all))
    boards = board_cards.T
    level_values, root, best = evaluate(
        up_weight,
        up_parent,
        root_parent[None, :],
        boards,
        opp_range[None, :],
        br_range[None, :],
        cards,
        opp_actions.T,
        leaf_kind.transpose(1, 2, 0).reshape(span, boards_dev),
        leaf_stake.transpose(1, 2, 0).reshape(span, boards_dev),
        br_actions,
        hand_rank,
        opp_weight.reshape(boards_dev, span, hands_dev),
        leafs,
        hands,
        actions,
    )
    return (level_values, root[0], best[0, 0])


def solution(mesh):
    in_specs = (
        P("hand"),
        P("hand"),
        P(None, "leaf", "hand"),
        P(),
        P("leaf", None),
        P("leaf", None),
        P("leaf"),
        P("leaf"),
        P("leaf", None),
        P("leaf", None, None),
        P("leaf", None, None),
        P("leaf", None, None, "hand"),
    )
    out_specs = (P(None, "leaf", "hand"), P("hand"), P())
    return jax.shard_map(local, mesh=mesh, in_specs=in_specs, out_specs=out_specs, check_vma=False)
```

```python
import functools

import jax
import jax.numpy as jnp
import numpy as np
from jax import lax
from jax.experimental import pallas as pl
from jax.experimental.pallas import tpu as pltpu
from jax.sharding import PartitionSpec as P

PAYOFF_UNIT = 1.0 / 4096.0
VMEM_LIMIT = 60 * 1024 * 1024
F32 = jnp.float32
BF16 = jnp.bfloat16


def hand_cards(number):
    low_list = []
    high_list = []
    for low_card in range(52):
        for high_card in range(low_card + 1, 52):
            low_list.append(low_card)
            high_list.append(high_card)
    chosen = np.arange(number) * 1326 // number
    cards = np.zeros((8, number), np.float32)
    cards[0] = np.array(low_list)[chosen]
    cards[1] = np.array(high_list)[chosen]
    cards[2] = np.exp2(np.arange(number) * 0.6180339887498949 % 1.0)
    cards[3] = 1.0 / cards[2]
    return cards


def vmem():
    return pl.BlockSpec(memory_space=pltpu.VMEM)


def hbm():
    return pl.BlockSpec(memory_space=pl.ANY)


def greet(axes_sizes):
    barrier = pltpu.get_barrier_semaphore()
    count = 0
    for axis, size in axes_sizes:
        me = lax.axis_index(axis)
        for dist in range(1, size):
            pl.semaphore_signal(
                barrier,
                inc=1,
                device_id={axis: lax.rem(me + dist, size)},
                device_id_type=pl.DeviceIdType.MESH,
            )
            count += 1
    pl.semaphore_wait(barrier, count)


def flip(index, mask):
    out = index
    bit = 1
    while bit <= mask:
        if mask & bit:
            out = out + bit - 2 * bit * lax.rem(index // bit, 2)
        bit *= 2
    return out


def peers_of(me, size):
    if size & (size - 1):
        return [lax.rem(me + dist, size) for dist in range(1, size)]
    far = [mask for mask in range(1, size) if mask >= size // 2]
    near = [mask for mask in range(1, size) if mask < size // 2]
    return [flip(me, mask) for mask in far + near]


def push(axis, peers, source, target, sem):
    for peer in peers:
        send(axis, peer, source(peer), target, sem).start()


def send(axis, peer, source, target, sem):
    send_sem, recv_sem = sem
    return pltpu.make_async_remote_copy(
        src_ref=source,
        dst_ref=target,
        send_sem=send_sem,
        recv_sem=recv_sem,
        device_id={axis: peer},
        device_id_type=pl.DeviceIdType.MESH,
    )


def settle(ref, sem):
    pltpu.make_async_copy(ref, ref, sem).wait()


def columns_of(ref, pad_ref):
    lines, count = ref.shape
    pad_ref[...] = jnp.zeros(pad_ref.shape, F32)
    pad_ref[0:lines, 0:count] = ref[...].astype(F32)
    return pad_ref[...].T


def kernel(
    leafs, hands, levels, actions,
    upper_ref, parent_ref, root_ref, board_ref, range_ref, br_ref, cards_ref, opp_ref, kind_ref, stake_ref,
    actions_ref, rank_ref, weight_ref,
    level_out, root_out, best_out,
    every, weights, ranks_in, ratio, ratio_in, reach, reach_in, anc, anc_all, br_all,
    pad, board_columns, stake_lines, stake_rows, apart_ref, against_ref, scaled,
    ready, values_all, units, units_all,
    up_s, up_r, pass_r, anc_s, anc_r, ratio_s, ratio_r, reach_s, reach_r, br_s, br_r,
    value_s, value_r, unit_s, unit_r, load_sem, own_sem,
):
    leaf = lax.axis_index("leaf")
    hand = lax.axis_index("hand")
    count = ratio.shape[1] // (2 * actions)
    width = weights.shape[3]
    boards = hands * count
    chunks = count // 8
    all_hands = hands * width
    span = actions * actions
    both = 2 * actions
    nodes_dev = upper_ref.shape[1]
    nodes = leafs * nodes_dev
    partners = peers_of(hand, hands)
    others = [lax.rem(leaf + dist, leafs) for dist in range(1, leafs)]

    def load(part, chunk):
        first = pl.multiple_of(part * count + chunk * 8, 8)
        return pltpu.make_async_copy(
            weight_ref.at[pl.ds(first, 8)], weights.at[part, pl.ds(chunk * 8, 8)], load_sem.at[chunk]
        )

    parts = partners + [hand]
    for chunk in range(chunks):
        for part in parts:
            load(part, chunk).start()
    own_upper = pltpu.make_async_copy(upper_ref, every.at[leaf], own_sem.at[0])
    own_upper.start()
    own_ranks = pltpu.make_async_copy(
        rank_ref.at[pl.ds(pl.multiple_of(hand * count, 8), count)], ranks_in, own_sem.at[1]
    )
    own_ranks.start()
    greet((("leaf", leafs), ("hand", hands)))
    ring = leafs // 2
    side = lax.rem(leaf, 2)
    twin = leaf + 1 - 2 * side

    def up_copy(source, owner, peer, k):
        return pltpu.make_async_remote_copy(
            src_ref=source,
            dst_ref=every.at[owner],
            send_sem=up_s,
            recv_sem=pass_r if k is None else up_r.at[k],
            device_id={"leaf": peer},
            device_id_type=pl.DeviceIdType.MESH,
        )

    def around(dist):
        return lax.rem(leaf // 2 + dist, ring) * 2 + side

    steps = sorted(range(1, ring), key=lambda dist: min(dist, ring - dist))
    up_direct = {dist: up_copy(upper_ref, leaf, around(dist), dist) for dist in steps}
    up_direct[0] = up_copy(upper_ref, leaf, twin, 0)
    for dist in steps + [0]:
        up_direct[dist].start()

    def pass_on(dists):
        for dist in dists:
            up_direct[dist].wait_recv()
            origin = around(ring - dist)
            up_copy(every.at[origin], origin, twin, None).start()

    stake_lines[...] = jnp.zeros(stake_lines.shape, F32)
    reply_ids = lax.broadcasted_iota(jnp.int32, (actions, boards), 0)
    for a in range(actions):
        lines = slice(a * actions, (a + 1) * actions)
        stake = stake_ref[lines, :]
        signed = jnp.where(kind_ref[lines, :] == 1, stake, -stake)
        legal = reply_ids < opp_ref[a : a + 1, :]
        stake_lines[lines, 0:boards] = jnp.where(legal, signed, 0).astype(F32)
    stake_rows[...] = stake_lines[...].T

    diagonal = lax.broadcasted_iota(jnp.int32, (actions, span), 0) == (
        lax.broadcasted_iota(jnp.int32, (actions, span), 1) // actions
    )
    own_lanes = pl.ds(pl.multiple_of(hand * width, width), width)
    spread = cards_ref[2:3, own_lanes]

    def fold(part, chunk, target):
        lines = stake_rows[pl.ds(pl.multiple_of(part * count + chunk * 8, 8), 8), :]
        for i in range(8):
            stake = jnp.broadcast_to(lines[i : i + 1, :], (actions, span))
            stake = jnp.where(diagonal, stake, 0.0)
            legal = jnp.where(stake != 0.0, 1.0, 0.0)
            shown = jnp.maximum(stake, 0.0)
            folds = jnp.maximum(-stake, 0.0)
            shown_hi = jnp.floor(shown * 0.5) * 2.0
            fold_hi = jnp.floor(folds * 0.5) * 2.0
            rows = jnp.concatenate([legal, shown_hi, shown - shown_hi, fold_hi, folds - fold_hi], axis=0)
            sums = jnp.dot(rows.astype(BF16), weights[part, chunk * 8 + i], preferred_element_type=F32)
            piece = [sums[j * actions : (j + 1) * actions] for j in range(5)]
            scale = spread / piece[0]
            pair = jnp.concatenate(
                [(piece[1] + piece[2]) * scale, (piece[3] + piece[4]) * scale], axis=0
            )
            place = (chunk * 8 + i) * both
            target[part, place : place + both, :] = pair.astype(BF16)

    for chunk in range(chunks):
        block = pl.ds(chunk * 8 * both, 8 * both)
        settle(weights.at[:, pl.ds(chunk * 8, 8)], load_sem.at[chunk])
        for part in partners:
            fold(part, chunk, ratio)
            send(
                "hand", part, ratio.at[part, block], ratio_in.at[hand, block], (ratio_s, ratio_r.at[chunk])
            ).start()
    push("hand", partners, lambda peer: br_ref, br_all.at[hand], (br_s, br_r))
    br_all[hand] = br_ref[...]

    node_column = lax.broadcasted_iota(jnp.int32, (nodes, boards), 0)
    pad[...] = jnp.zeros(pad.shape, F32)
    line = root_ref[...]
    pad[levels - 1 : levels, 0:boards] = line.astype(F32)
    for level in range(levels - 2, -1, -1):
        parents = jnp.broadcast_to(parent_ref[level : level + 1, :], (8, nodes)).astype(F32)
        column = parents.T[:, 0:1]
        line_f = jnp.sum(jnp.where(node_column == line, column, 0.0), axis=0, keepdims=True)
        pad[level : level + 1, 0:boards] = line_f
        line = line_f.astype(jnp.int32)
    anc_float = pad[...].T
    anc_columns = anc_float.astype(jnp.int32)
    lane = lax.broadcasted_iota(jnp.int32, (boards, boards), 1)
    held = (lane % (hands * 8)) // 8 * count + lane // (hands * 8) * 8 + lane % 8
    moved = lax.broadcasted_iota(jnp.int32, (boards, boards), 0) == held
    anc[...] = jnp.zeros(anc.shape, F32)
    for level in range(levels):
        anc[level : level + 1, 0:boards] = jnp.sum(
            jnp.where(moved, anc_float[0:boards, level : level + 1], 0.0), axis=0, keepdims=True
        )
    push("leaf", others, lambda peer: anc, anc_all.at[leaf], (anc_s, anc_r))
    anc_all[leaf] = anc[...]

    low = cards_ref[0:1, :]
    high = cards_ref[1:2, :]
    card_columns = cards_ref[...].T
    for part in range(hands):
        if part == hands // 2:
            pass_on([dist for dist in steps if dist in (1, ring - 1)])
        rows = slice(part * width, (part + 1) * width)
        low_col = card_columns[rows, 0:1]
        high_col = card_columns[rows, 1:2]
        hit = (low_col == low) | (low_col == high) | (high_col == low) | (high_col == high)
        apart_ref[rows, :] = jnp.where(hit, 0.0, 1.0).astype(BF16)
        against_ref[rows, :] = jnp.where(hit, 0.0, -1.0).astype(BF16)

    pass_on([dist for dist in steps if dist not in (1, ring - 1)])
    for chunk in range(chunks):
        fold(hand, chunk, ratio_in)

    own_low = cards_ref[0:1, own_lanes]
    own_high = cards_ref[1:2, own_lanes]
    board_columns[...] = columns_of(board_ref, pad)
    free = jnp.ones((boards, width), F32)
    for card in range(5):
        column = board_columns[0:boards, card : card + 1]
        free = jnp.where((column == own_low) | (column == own_high), 0.0, free)
    free = free * cards_ref[3:4, own_lanes]

    own_ranks.wait()
    ranks = ((ranks_in[...] % 128) + 128).astype(F32)
    octave = ranks_in[...] // 128
    for bit in (1, 2, 4, 8, 16, 32):
        ranks = ranks * jnp.where(octave // bit % 2 == 1, float(2**bit), 1.0)
    scaled[...] = ranks

    own_upper.wait()
    up_direct[0].wait_recv()
    settle(every.at[pl.ds(0, ring - 1)], pass_r)
    settle(every.at[pl.ds(0, leafs - 1)], up_s)
    node_ids = lax.broadcasted_iota(jnp.int32, (boards, nodes), 1)
    total = jnp.broadcast_to(range_ref[...], (boards, width))
    for level in range(levels):
        pick = jnp.where(anc_columns[0:boards, level : level + 1] == node_ids, 1.0, 0.0).astype(BF16)
        table = every[:, level].reshape(nodes, width)
        total = total * jnp.dot(pick, table, preferred_element_type=F32)
    total = total * free
    for part in range(hands):
        for chunk in range(chunks):
            first = part * count + chunk * 8
            reach[part, chunk] = total[first : first + 8].astype(BF16)
    push("hand", partners, lambda peer: reach.at[peer], reach_in.at[hand], (reach_s, reach_r))
    reach_in[hand] = reach[hand]
    action_ids = lax.broadcasted_iota(jnp.int32, (actions, 1), 0)
    settle(br_all.at[pl.ds(0, hands - 1)], br_r)
    br_row = jnp.concatenate([br_all[part] for part in range(hands)], axis=1)
    settle(reach.at[pl.ds(0, hands - 1)], reach_r)

    def values(chunk):
        first = pl.multiple_of(hand * count + chunk * 8, 8)
        cards_on = board_columns[pl.ds(first, 8), :]
        open_hands = jnp.ones((8, all_hands), F32)
        for card in range(5):
            column = cards_on[:, card : card + 1]
            open_hands = jnp.where((column == low) | (column == high), 0.0, open_hands)
        rank_rows = scaled[pl.ds(pl.multiple_of(chunk * 8, 8), 8), :]
        rank_columns = rank_rows.T.astype(BF16)
        rank_rows = rank_rows.astype(BF16)
        lines = []
        folded = jnp.zeros((8 * both, all_hands), F32)
        for part in range(hands):
            pieces = []
            reach_rows = reach_in[part, chunk].astype(F32)
            for i in range(8):
                b = chunk * 8 + i
                row = ratio_in[part, pl.ds(pl.multiple_of(b * both, both), both), :].astype(F32)
                pieces.append((row * reach_rows[i : i + 1, :]).astype(BF16))
            lines.append(pieces)
            folded = folded + jnp.dot(
                jnp.concatenate(pieces, axis=0),
                apart_ref[part * width : (part + 1) * width, :],
                preferred_element_type=F32,
            )
        best_rows = []
        for i in range(8):
            shown = jnp.zeros((both, all_hands), F32)
            for part in range(hands):
                rows = slice(part * width, (part + 1) * width)
                order = rank_rows[i : i + 1, :] - rank_columns[rows, i : i + 1]
                order = jnp.minimum(jnp.maximum(order, against_ref[rows, :]), apart_ref[rows, :])
                shown = shown + jnp.dot(lines[part][i], order, preferred_element_type=F32)
            per_node = shown[0:actions] + folded[i * both + actions : (i + 1) * both]
            allowed = action_ids < actions_ref[first + i]
            best_rows.append(jnp.max(jnp.where(allowed, per_node, -1e30), axis=0, keepdims=True))
        best = jnp.concatenate(best_rows, axis=0) * (open_hands * PAYOFF_UNIT)
        peak = jnp.max(jnp.abs(best), axis=1, keepdims=True) * (1.0 / 32640.0)
        unit = jnp.full((8, 1), 2.0**16, F32)
        inverse = jnp.full((8, 1), 2.0**-16, F32)
        for bit in (64, 32, 16, 8, 4, 2, 1):
            fits = peak <= unit * 2.0**-bit
            unit = jnp.where(fits, unit * 2.0**-bit, unit)
            inverse = jnp.where(fits, inverse * 2.0**bit, inverse)
        codes = jnp.floor(best * inverse + 0.5).astype(jnp.int32).astype(jnp.int16)
        for part in range(hands):
            ready[chunk, part] = codes[:, part * width : (part + 1) * width]
        share = jnp.sum(jnp.sum(best * br_row, axis=1, keepdims=True), axis=0, keepdims=True)
        lane = lax.broadcasted_iota(jnp.int32, (8, 128), 1)
        place = hand * 8 + lax.broadcasted_iota(jnp.int32, (8, 128), 0)
        row = jnp.sum(jnp.where(lane == place, unit, 0.0), axis=0, keepdims=True)
        units[chunk] = jnp.where(lane[0:1] == hands * 8, share, row)

    peers = leafs * hands

    def send_values(chunk, k):
        to_hand = lax.rem(hand + k % hands, hands)
        target = {"leaf": lax.rem(leaf + k // hands, leafs), "hand": to_hand}
        pltpu.make_async_remote_copy(
            src_ref=ready.at[chunk, to_hand],
            dst_ref=values_all.at[chunk, leaf * hands + hand],
            send_sem=value_s,
            recv_sem=value_r.at[chunk],
            device_id=target,
            device_id_type=pl.DeviceIdType.MESH,
        ).start()
        pltpu.make_async_remote_copy(
            src_ref=units.at[chunk],
            dst_ref=units_all.at[chunk, leaf * hands + hand],
            send_sem=unit_s,
            recv_sem=unit_r.at[chunk],
            device_id=target,
            device_id_type=pl.DeviceIdType.MESH,
        ).start()

    def one_chunk(chunk, carry):
        settle(ratio.at[pl.ds(0, hands - 1), pl.ds(0, 8 * both)], ratio_r.at[chunk])
        values(chunk)

        def one(k, carry):
            send_values(chunk, k)
            return carry

        lax.fori_loop(1, peers, one, 0, unroll=peers <= 32)
        values_all[chunk, leaf * hands + hand] = ready[chunk, hand]
        units_all[chunk, leaf * hands + hand] = units[chunk]
        return carry

    lax.fori_loop(0, chunks, one_chunk, 0)
    settle(ratio.at[pl.ds(0, hands - 1)], ratio_s)
    settle(reach.at[pl.ds(0, hands - 1)], reach_s)
    settle(br_all.at[pl.ds(0, hands - 1)], br_s)

    settle(anc_all.at[pl.ds(0, leafs - 1)], anc_r)
    settle(anc_all.at[pl.ds(0, leafs - 1)], anc_s)
    lines_dev = levels * nodes_dev
    block = hands * 8
    node_rows = leaf * nodes_dev + lax.broadcasted_iota(jnp.int32, (nodes_dev, block), 0)
    node_rows = node_rows.astype(F32)

    def add_leaf(chunk, source, sums):
        own = pl.ds(source * hands, hands)
        part = values_all[chunk, own].astype(jnp.int32).astype(F32).reshape(block, width)
        coarse = part.astype(BF16)
        fine = (part - coarse.astype(F32)).astype(BF16)
        lines = anc_all[source][:, chunk * block : (chunk + 1) * block]
        row = jnp.sum(units_all[chunk, own], axis=0)
        unit = row[:, 0:block]
        pick = [jnp.where(lines[k : k + 1, :] == node_rows, unit, 0.0) for k in range(levels)]
        pick = jnp.concatenate(pick + [jnp.broadcast_to(unit, (8, block))], axis=0).astype(BF16)
        sums = sums + jnp.dot(pick, coarse, preferred_element_type=F32)
        return sums + jnp.dot(pick, fine, preferred_element_type=F32), row[:, block : block + 1]

    sums = jnp.zeros((lines_dev + 8, width), F32)
    whole = jnp.zeros((1, 1), F32)
    for chunk in range(chunks):
        settle(values_all.at[chunk, pl.ds(0, peers - 1)], value_r.at[chunk])
        settle(units_all.at[chunk, pl.ds(0, peers - 1)], unit_r.at[chunk])
        for source in range(leafs):
            sums, share = add_leaf(chunk, source, sums)
            whole = whole + share
    root_out[...] = sums[lines_dev : lines_dev + 1] / nodes
    for k in range(levels):
        level_out[k] = sums[k * nodes_dev : (k + 1) * nodes_dev]
    for chunk in range(chunks):
        settle(values_all.at[chunk, pl.ds(0, peers - 1)], value_s)
        settle(units_all.at[chunk, pl.ds(0, peers - 1)], unit_s)
    best_out[...] = whole / nodes / jnp.sum(br_row, axis=1, keepdims=True)


def evaluate(
    upper, parents, roots, boards, opp_range, br_range, cards, opp_actions, kinds, stakes,
    br_actions, ranks, weights, leafs, hands, actions,
):
    levels, nodes_dev, width = upper.shape
    boards_dev, span, _ = weights.shape
    count = boards_dev // hands
    chunks = count // 8
    both = 2 * actions
    all_hands = ranks.shape[1]
    lanes = -(-boards_dev // 128) * 128
    dma = pltpu.SemaphoreType.DMA
    return pl.pallas_call(
        functools.partial(kernel, leafs, hands, levels, actions),
        out_shape=(
            jax.ShapeDtypeStruct((levels, nodes_dev, width), F32),
            jax.ShapeDtypeStruct((1, width), F32),
            jax.ShapeDtypeStruct((1, 1), F32),
        ),
        in_specs=[vmem()] * 10 + [pl.BlockSpec(memory_space=pltpu.SMEM), hbm(), hbm()],
        out_specs=(vmem(), vmem(), vmem()),
        scratch_shapes=[
            pltpu.VMEM((leafs, levels, nodes_dev, width), BF16),
            pltpu.VMEM((hands, count, span, width), BF16),
            pltpu.VMEM((count, all_hands), jnp.int32),
            pltpu.VMEM((hands, count * both, width), BF16),
            pltpu.VMEM((hands, count * both, width), BF16),
            pltpu.VMEM((hands, chunks, 8, width), BF16),
            pltpu.VMEM((hands, chunks, 8, width), BF16),
            pltpu.VMEM((8, lanes), F32),
            pltpu.VMEM((leafs, 8, lanes), F32),
            pltpu.VMEM((hands, 1, width), F32),
            pltpu.VMEM((8, lanes), F32),
            pltpu.VMEM((lanes, 8), F32),
            pltpu.VMEM((span, lanes), F32),
            pltpu.VMEM((lanes, span), F32),
            pltpu.VMEM((all_hands, all_hands), BF16),
            pltpu.VMEM((all_hands, all_hands), BF16),
            pltpu.VMEM((count, all_hands), F32),
            pltpu.VMEM((chunks, hands, 8, width), jnp.int16),
            pltpu.VMEM((chunks, leafs * hands, 8, width), jnp.int16),
            pltpu.VMEM((chunks, 1, 128), F32),
            pltpu.VMEM((chunks, leafs * hands, 1, 128), F32),
            dma(()), dma((max(leafs // 2, 1),)), dma(()), dma(()), dma(()),
            dma(()), dma((chunks,)), dma(()), dma(()), dma(()), dma(()),
            dma(()), dma((chunks,)), dma(()), dma((chunks,)),
            dma((chunks,)), dma((2,)),
        ],
        compiler_params=pltpu.CompilerParams(
            collective_id=0, has_side_effects=True, vmem_limit_bytes=VMEM_LIMIT
        ),
        name="evaluate",
    )(
        upper, parents, roots, boards, opp_range, br_range, cards, opp_actions, kinds, stakes,
        br_actions, ranks, weights,
    )


def local(
    opp_range,
    br_range,
    up_weight,
    up_parent,
    board_cards,
    hand_rank,
    root_parent,
    br_actions,
    opp_actions,
    leaf_kind,
    leaf_stake,
    opp_weight,
):
    hands_dev = up_weight.shape[2]
    boards_dev, hands_all = hand_rank.shape
    actions = opp_actions.shape[1]
    span = actions * actions
    leafs = lax.axis_size("leaf")
    hands = lax.axis_size("hand")
    cards = jnp.asarray(hand_cards(hands_all))
    boards = board_cards.T
    level_values, root, best = evaluate(
        up_weight,
        up_parent,
        root_parent[None, :],
        boards,
        opp_range[None, :],
        br_range[None, :],
        cards,
        opp_actions.T,
        leaf_kind.transpose(1, 2, 0).reshape(span, boards_dev),
        leaf_stake.transpose(1, 2, 0).reshape(span, boards_dev),
        br_actions,
        hand_rank,
        opp_weight.reshape(boards_dev, span, hands_dev),
        leafs,
        hands,
        actions,
    )
    return (level_values, root[0], best[0, 0])


def solution(mesh):
    in_specs = (
        P("hand"),
        P("hand"),
        P(None, "leaf", "hand"),
        P(),
        P("leaf", None),
        P("leaf", None),
        P("leaf"),
        P("leaf"),
        P("leaf", None),
        P("leaf", None, None),
        P("leaf", None, None),
        P("leaf", None, None, "hand"),
    )
    out_specs = (P(None, "leaf", "hand"), P("hand"), P())
    return jax.shard_map(local, mesh=mesh, in_specs=in_specs, out_specs=out_specs, check_vma=False)
```

```python
import functools

import jax
import jax.numpy as jnp
import numpy as np
from jax import lax
from jax.experimental import pallas as pl
from jax.experimental.pallas import tpu as pltpu
from jax.sharding import PartitionSpec as P

PAYOFF_UNIT = 1.0 / 4096.0
VMEM_LIMIT = 60 * 1024 * 1024
F32 = jnp.float32
BF16 = jnp.bfloat16


def hand_cards(number):
    low_list = []
    high_list = []
    for low_card in range(52):
        for high_card in range(low_card + 1, 52):
            low_list.append(low_card)
            high_list.append(high_card)
    chosen = np.arange(number) * 1326 // number
    cards = np.zeros((8, number), np.float32)
    cards[0] = np.array(low_list)[chosen]
    cards[1] = np.array(high_list)[chosen]
    cards[2] = np.exp2(np.arange(number) * 0.6180339887498949 % 1.0)
    cards[3] = 1.0 / cards[2]
    return cards


def vmem():
    return pl.BlockSpec(memory_space=pltpu.VMEM)


def hbm():
    return pl.BlockSpec(memory_space=pl.ANY)


def greet(axes_sizes):
    barrier = pltpu.get_barrier_semaphore()
    count = 0
    for axis, size in axes_sizes:
        me = lax.axis_index(axis)
        for dist in range(1, size):
            pl.semaphore_signal(
                barrier,
                inc=1,
                device_id={axis: lax.rem(me + dist, size)},
                device_id_type=pl.DeviceIdType.MESH,
            )
            count += 1
    pl.semaphore_wait(barrier, count)


def flip(index, mask):
    out = index
    bit = 1
    while bit <= mask:
        if mask & bit:
            out = out + bit - 2 * bit * lax.rem(index // bit, 2)
        bit *= 2
    return out


def peers_of(me, size):
    if size & (size - 1):
        return [lax.rem(me + dist, size) for dist in range(1, size)]
    far = [mask for mask in range(1, size) if mask >= size // 2]
    near = [mask for mask in range(1, size) if mask < size // 2]
    return [flip(me, mask) for mask in far + near]


def push(axis, peers, source, target, sem):
    for peer in peers:
        send(axis, peer, source(peer), target, sem).start()


def send(axis, peer, source, target, sem):
    send_sem, recv_sem = sem
    return pltpu.make_async_remote_copy(
        src_ref=source,
        dst_ref=target,
        send_sem=send_sem,
        recv_sem=recv_sem,
        device_id={axis: peer},
        device_id_type=pl.DeviceIdType.MESH,
    )


def settle(ref, sem):
    pltpu.make_async_copy(ref, ref, sem).wait()


def columns_of(ref, pad_ref):
    lines, count = ref.shape
    pad_ref[...] = jnp.zeros(pad_ref.shape, F32)
    pad_ref[0:lines, 0:count] = ref[...].astype(F32)
    return pad_ref[...].T


def kernel(
    leafs, hands, levels, actions,
    upper_ref, parent_ref, root_ref, board_ref, range_ref, br_ref, cards_ref, opp_ref, kind_ref, stake_ref,
    actions_ref, rank_ref, weight_ref,
    flat_out,
    every, weights, ranks_in, ratio, ratio_in, reach, reach_in, anc, anc_all, br_all,
    pad, board_columns, stake_lines, stake_rows, apart_ref, against_ref, scaled,
    ready, values_all, units, units_all,
    up_s, up_r, pass_r, anc_s, anc_r, ratio_s, ratio_r, reach_s, reach_r, br_s, br_r,
    value_s, value_r, unit_s, unit_r, load_sem, own_sem,
):
    leaf = lax.axis_index("leaf")
    hand = lax.axis_index("hand")
    count = ratio.shape[1] // (2 * actions)
    width = weights.shape[3]
    boards = hands * count
    chunks = count // 8
    all_hands = hands * width
    span = actions * actions
    both = 2 * actions
    nodes_dev = upper_ref.shape[1]
    nodes = leafs * nodes_dev
    partners = peers_of(hand, hands)
    others = [lax.rem(leaf + dist, leafs) for dist in range(1, leafs)]

    def load(part, chunk):
        first = pl.multiple_of(part * count + chunk * 8, 8)
        return pltpu.make_async_copy(
            weight_ref.at[pl.ds(first, 8)], weights.at[part, pl.ds(chunk * 8, 8)], load_sem.at[chunk]
        )

    parts = partners + [hand]
    for chunk in range(chunks):
        for part in parts:
            load(part, chunk).start()
    own_upper = pltpu.make_async_copy(upper_ref, every.at[leaf], own_sem.at[0])
    own_upper.start()
    own_ranks = pltpu.make_async_copy(
        rank_ref.at[pl.ds(pl.multiple_of(hand * count, 8), count)], ranks_in, own_sem.at[1]
    )
    own_ranks.start()
    greet((("leaf", leafs), ("hand", hands)))
    ring = leafs // 2
    side = lax.rem(leaf, 2)
    twin = leaf + 1 - 2 * side

    def up_copy(source, owner, peer, k):
        return pltpu.make_async_remote_copy(
            src_ref=source,
            dst_ref=every.at[owner],
            send_sem=up_s,
            recv_sem=pass_r if k is None else up_r.at[k],
            device_id={"leaf": peer},
            device_id_type=pl.DeviceIdType.MESH,
        )

    def around(dist):
        return lax.rem(leaf // 2 + dist, ring) * 2 + side

    steps = sorted(range(1, ring), key=lambda dist: min(dist, ring - dist))
    up_direct = {dist: up_copy(upper_ref, leaf, around(dist), dist) for dist in steps}
    up_direct[0] = up_copy(upper_ref, leaf, twin, 0)
    for dist in steps + [0]:
        up_direct[dist].start()

    def pass_on(dists):
        for dist in dists:
            up_direct[dist].wait_recv()
            origin = around(ring - dist)
            up_copy(every.at[origin], origin, twin, None).start()

    stake_lines[...] = jnp.zeros(stake_lines.shape, F32)
    reply_ids = lax.broadcasted_iota(jnp.int32, (actions, boards), 0)
    for a in range(actions):
        lines = slice(a * actions, (a + 1) * actions)
        stake = stake_ref[lines, :]
        signed = jnp.where(kind_ref[lines, :] == 1, stake, -stake)
        legal = reply_ids < opp_ref[a : a + 1, :]
        stake_lines[lines, 0:boards] = jnp.where(legal, signed, 0).astype(F32)
    stake_rows[...] = stake_lines[...].T

    diagonal = lax.broadcasted_iota(jnp.int32, (actions, span), 0) == (
        lax.broadcasted_iota(jnp.int32, (actions, span), 1) // actions
    )
    own_lanes = pl.ds(pl.multiple_of(hand * width, width), width)
    spread = cards_ref[2:3, own_lanes]

    def fold(part, chunk, target):
        lines = stake_rows[pl.ds(pl.multiple_of(part * count + chunk * 8, 8), 8), :]
        for i in range(8):
            stake = jnp.broadcast_to(lines[i : i + 1, :], (actions, span))
            stake = jnp.where(diagonal, stake, 0.0)
            legal = jnp.where(stake != 0.0, 1.0, 0.0)
            shown = jnp.maximum(stake, 0.0)
            folds = jnp.maximum(-stake, 0.0)
            shown_hi = jnp.floor(shown * 0.5) * 2.0
            fold_hi = jnp.floor(folds * 0.5) * 2.0
            rows = jnp.concatenate([legal, shown_hi, shown - shown_hi, fold_hi, folds - fold_hi], axis=0)
            sums = jnp.dot(rows.astype(BF16), weights[part, chunk * 8 + i], preferred_element_type=F32)
            piece = [sums[j * actions : (j + 1) * actions] for j in range(5)]
            scale = spread / piece[0]
            pair = jnp.concatenate(
                [(piece[1] + piece[2]) * scale, (piece[3] + piece[4]) * scale], axis=0
            )
            place = (chunk * 8 + i) * both
            target[part, place : place + both, :] = pair.astype(BF16)

    for chunk in range(chunks):
        block = pl.ds(chunk * 8 * both, 8 * both)
        settle(weights.at[:, pl.ds(chunk * 8, 8)], load_sem.at[chunk])
        for part in partners:
            fold(part, chunk, ratio)
            send(
                "hand", part, ratio.at[part, block], ratio_in.at[hand, block], (ratio_s, ratio_r.at[chunk])
            ).start()
    push("hand", partners, lambda peer: br_ref, br_all.at[hand], (br_s, br_r))
    br_all[hand] = br_ref[...]

    node_column = lax.broadcasted_iota(jnp.int32, (nodes, boards), 0)
    pad[...] = jnp.zeros(pad.shape, F32)
    line = root_ref[...]
    pad[levels - 1 : levels, 0:boards] = line.astype(F32)
    for level in range(levels - 2, -1, -1):
        parents = jnp.broadcast_to(parent_ref[level : level + 1, :], (8, nodes)).astype(F32)
        column = parents.T[:, 0:1]
        line_f = jnp.sum(jnp.where(node_column == line, column, 0.0), axis=0, keepdims=True)
        pad[level : level + 1, 0:boards] = line_f
        line = line_f.astype(jnp.int32)
    anc_float = pad[...].T
    anc_columns = anc_float.astype(jnp.int32)
    lane = lax.broadcasted_iota(jnp.int32, (boards, boards), 1)
    held = (lane % (hands * 8)) // 8 * count + lane // (hands * 8) * 8 + lane % 8
    moved = lax.broadcasted_iota(jnp.int32, (boards, boards), 0) == held
    anc[...] = jnp.zeros(anc.shape, F32)
    for level in range(levels):
        anc[level : level + 1, 0:boards] = jnp.sum(
            jnp.where(moved, anc_float[0:boards, level : level + 1], 0.0), axis=0, keepdims=True
        )
    push("leaf", others, lambda peer: anc, anc_all.at[leaf], (anc_s, anc_r))
    anc_all[leaf] = anc[...]

    low = cards_ref[0:1, :]
    high = cards_ref[1:2, :]
    card_columns = cards_ref[...].T
    for part in range(hands):
        if part == hands // 2:
            pass_on([dist for dist in steps if dist in (1, ring - 1)])
        rows = slice(part * width, (part + 1) * width)
        low_col = card_columns[rows, 0:1]
        high_col = card_columns[rows, 1:2]
        hit = (low_col == low) | (low_col == high) | (high_col == low) | (high_col == high)
        apart_ref[rows, :] = jnp.where(hit, 0.0, 1.0).astype(BF16)
        against_ref[rows, :] = jnp.where(hit, 0.0, -1.0).astype(BF16)

    pass_on([dist for dist in steps if dist not in (1, ring - 1)])
    for chunk in range(chunks):
        fold(hand, chunk, ratio_in)

    own_low = cards_ref[0:1, own_lanes]
    own_high = cards_ref[1:2, own_lanes]
    board_columns[...] = columns_of(board_ref, pad)
    free = jnp.ones((boards, width), F32)
    for card in range(5):
        column = board_columns[0:boards, card : card + 1]
        free = jnp.where((column == own_low) | (column == own_high), 0.0, free)
    free = free * cards_ref[3:4, own_lanes]

    own_ranks.wait()
    ranks = ((ranks_in[...] % 128) + 128).astype(F32)
    octave = ranks_in[...] // 128
    for bit in (1, 2, 4, 8, 16, 32):
        ranks = ranks * jnp.where(octave // bit % 2 == 1, float(2**bit), 1.0)
    scaled[...] = ranks

    own_upper.wait()
    up_direct[0].wait_recv()
    settle(every.at[pl.ds(0, ring - 1)], pass_r)
    settle(every.at[pl.ds(0, leafs - 1)], up_s)
    node_ids = lax.broadcasted_iota(jnp.int32, (boards, nodes), 1)
    total = jnp.broadcast_to(range_ref[...], (boards, width))
    for level in range(levels):
        pick = jnp.where(anc_columns[0:boards, level : level + 1] == node_ids, 1.0, 0.0).astype(BF16)
        table = every[:, level].reshape(nodes, width)
        total = total * jnp.dot(pick, table, preferred_element_type=F32)
    total = total * free
    for part in range(hands):
        for chunk in range(chunks):
            first = part * count + chunk * 8
            reach[part, chunk] = total[first : first + 8].astype(BF16)
    push("hand", partners, lambda peer: reach.at[peer], reach_in.at[hand], (reach_s, reach_r))
    reach_in[hand] = reach[hand]
    action_ids = lax.broadcasted_iota(jnp.int32, (actions, 1), 0)
    settle(br_all.at[pl.ds(0, hands - 1)], br_r)
    br_row = jnp.concatenate([br_all[part] for part in range(hands)], axis=1)
    settle(reach.at[pl.ds(0, hands - 1)], reach_r)

    def values(chunk):
        first = pl.multiple_of(hand * count + chunk * 8, 8)
        cards_on = board_columns[pl.ds(first, 8), :]
        open_hands = jnp.ones((8, all_hands), F32)
        for card in range(5):
            column = cards_on[:, card : card + 1]
            open_hands = jnp.where((column == low) | (column == high), 0.0, open_hands)
        rank_rows = scaled[pl.ds(pl.multiple_of(chunk * 8, 8), 8), :]
        rank_columns = rank_rows.T.astype(BF16)
        rank_rows = rank_rows.astype(BF16)
        lines = []
        folded = jnp.zeros((8 * both, all_hands), F32)
        for part in range(hands):
            pieces = []
            reach_rows = reach_in[part, chunk].astype(F32)
            for i in range(8):
                b = chunk * 8 + i
                row = ratio_in[part, pl.ds(pl.multiple_of(b * both, both), both), :].astype(F32)
                pieces.append((row * reach_rows[i : i + 1, :]).astype(BF16))
            lines.append(pieces)
            folded = folded + jnp.dot(
                jnp.concatenate(pieces, axis=0),
                apart_ref[part * width : (part + 1) * width, :],
                preferred_element_type=F32,
            )
        best_rows = []
        for i in range(8):
            shown = jnp.zeros((both, all_hands), F32)
            for part in range(hands):
                rows = slice(part * width, (part + 1) * width)
                order = rank_rows[i : i + 1, :] - rank_columns[rows, i : i + 1]
                order = jnp.minimum(jnp.maximum(order, against_ref[rows, :]), apart_ref[rows, :])
                order = order.astype(jnp.float8_e4m3fn)
                shown = shown + jnp.dot(lines[part][i], order, preferred_element_type=F32)
            per_node = shown[0:actions] + folded[i * both + actions : (i + 1) * both]
            allowed = action_ids < actions_ref[first + i]
            best_rows.append(jnp.max(jnp.where(allowed, per_node, -1e30), axis=0, keepdims=True))
        best = jnp.concatenate(best_rows, axis=0) * (open_hands * PAYOFF_UNIT)
        peak = jnp.max(jnp.abs(best), axis=1, keepdims=True) * (1.0 / 32640.0)
        unit = jnp.full((8, 1), 2.0**16, F32)
        inverse = jnp.full((8, 1), 2.0**-16, F32)
        for bit in (64, 32, 16, 8, 4, 2, 1):
            fits = peak <= unit * 2.0**-bit
            unit = jnp.where(fits, unit * 2.0**-bit, unit)
            inverse = jnp.where(fits, inverse * 2.0**bit, inverse)
        codes = jnp.floor(best * inverse + 0.5).astype(jnp.int32).astype(jnp.int16)
        for part in range(hands):
            ready[chunk, part] = codes[:, part * width : (part + 1) * width]
        share = jnp.sum(jnp.sum(best * br_row, axis=1, keepdims=True), axis=0, keepdims=True)
        lane = lax.broadcasted_iota(jnp.int32, (8, 128), 1)
        place = hand * 8 + lax.broadcasted_iota(jnp.int32, (8, 128), 0)
        row = jnp.sum(jnp.where(lane == place, unit, 0.0), axis=0, keepdims=True)
        units[chunk] = jnp.where(lane[0:1] == hands * 8, share, row)

    peers = leafs * hands

    def send_values(chunk, k):
        to_hand = lax.rem(hand + k % hands, hands)
        target = {"leaf": lax.rem(leaf + k // hands, leafs), "hand": to_hand}
        pltpu.make_async_remote_copy(
            src_ref=ready.at[chunk, to_hand],
            dst_ref=values_all.at[chunk, leaf * hands + hand],
            send_sem=value_s,
            recv_sem=value_r.at[chunk],
            device_id=target,
            device_id_type=pl.DeviceIdType.MESH,
        ).start()
        pltpu.make_async_remote_copy(
            src_ref=units.at[chunk],
            dst_ref=units_all.at[chunk, leaf * hands + hand],
            send_sem=unit_s,
            recv_sem=unit_r.at[chunk],
            device_id=target,
            device_id_type=pl.DeviceIdType.MESH,
        ).start()

    def one_chunk(chunk, carry):
        settle(ratio.at[pl.ds(0, hands - 1), pl.ds(0, 8 * both)], ratio_r.at[chunk])
        values(chunk)

        def one(k, carry):
            send_values(chunk, k)
            return carry

        lax.fori_loop(1, peers, one, 0, unroll=peers <= 32)
        values_all[chunk, leaf * hands + hand] = ready[chunk, hand]
        units_all[chunk, leaf * hands + hand] = units[chunk]
        return carry

    lax.fori_loop(0, chunks, one_chunk, 0)
    settle(ratio.at[pl.ds(0, hands - 1)], ratio_s)
    settle(reach.at[pl.ds(0, hands - 1)], reach_s)
    settle(br_all.at[pl.ds(0, hands - 1)], br_s)

    settle(anc_all.at[pl.ds(0, leafs - 1)], anc_r)
    settle(anc_all.at[pl.ds(0, leafs - 1)], anc_s)
    lines_dev = levels * nodes_dev
    block = hands * 8
    node_rows = leaf * nodes_dev + lax.broadcasted_iota(jnp.int32, (nodes_dev, block), 0)
    node_rows = node_rows.astype(F32)

    def add_leaf(chunk, source, sums):
        own = pl.ds(source * hands, hands)
        part = values_all[chunk, own].astype(jnp.int32).astype(F32).reshape(block, width)
        coarse = part.astype(BF16)
        fine = (part - coarse.astype(F32)).astype(BF16)
        lines = anc_all[source][:, chunk * block : (chunk + 1) * block]
        row = jnp.sum(units_all[chunk, own], axis=0)
        unit = row[:, 0:block]
        pick = [jnp.where(lines[k : k + 1, :] == node_rows, unit, 0.0) for k in range(levels)]
        pick = jnp.concatenate(pick + [jnp.broadcast_to(unit, (8, block))], axis=0).astype(BF16)
        sums = sums + jnp.dot(pick, coarse, preferred_element_type=F32)
        return sums + jnp.dot(pick, fine, preferred_element_type=F32), row[:, block : block + 1]

    sums = jnp.zeros((lines_dev + 8, width), F32)
    whole = jnp.zeros((1, 1), F32)
    for chunk in range(chunks):
        settle(values_all.at[chunk, pl.ds(0, peers - 1)], value_r.at[chunk])
        settle(units_all.at[chunk, pl.ds(0, peers - 1)], unit_r.at[chunk])
        for source in range(leafs):
            sums, share = add_leaf(chunk, source, sums)
            whole = whole + share
    flat_out[0:lines_dev] = sums[0:lines_dev]
    for chunk in range(chunks):
        settle(values_all.at[chunk, pl.ds(0, peers - 1)], value_s)
        settle(units_all.at[chunk, pl.ds(0, peers - 1)], unit_s)
    best = whole / nodes / jnp.sum(br_row, axis=1, keepdims=True)
    line = lax.broadcasted_iota(jnp.int32, (8, width), 0)
    flat_out[lines_dev:] = jnp.where(line == 0, sums[lines_dev:] / nodes, best)


def spread_kernel(flat_ref, level_out, root_out, best_out):
    levels, nodes_dev, _ = level_out.shape
    for k in range(levels):
        level_out[k] = flat_ref[k * nodes_dev : (k + 1) * nodes_dev]
    root_out[...] = flat_ref[levels * nodes_dev]
    best_out[0, 0] = flat_ref[levels * nodes_dev + 1, 0]


def evaluate(
    upper, parents, roots, boards, opp_range, br_range, cards, opp_actions, kinds, stakes,
    br_actions, ranks, weights, leafs, hands, actions,
):
    levels, nodes_dev, width = upper.shape
    boards_dev, span, _ = weights.shape
    count = boards_dev // hands
    chunks = count // 8
    both = 2 * actions
    all_hands = ranks.shape[1]
    lanes = -(-boards_dev // 128) * 128
    dma = pltpu.SemaphoreType.DMA
    flat = pl.pallas_call(
        functools.partial(kernel, leafs, hands, levels, actions),
        out_shape=jax.ShapeDtypeStruct((levels * nodes_dev + 8, width), F32),
        in_specs=[vmem()] * 10 + [pl.BlockSpec(memory_space=pltpu.SMEM), hbm(), hbm()],
        out_specs=vmem(),
        scratch_shapes=[
            pltpu.VMEM((leafs, levels, nodes_dev, width), BF16),
            pltpu.VMEM((hands, count, span, width), BF16),
            pltpu.VMEM((count, all_hands), jnp.int32),
            pltpu.VMEM((hands, count * both, width), BF16),
            pltpu.VMEM((hands, count * both, width), BF16),
            pltpu.VMEM((hands, chunks, 8, width), BF16),
            pltpu.VMEM((hands, chunks, 8, width), BF16),
            pltpu.VMEM((8, lanes), F32),
            pltpu.VMEM((leafs, 8, lanes), F32),
            pltpu.VMEM((hands, 1, width), F32),
            pltpu.VMEM((8, lanes), F32),
            pltpu.VMEM((lanes, 8), F32),
            pltpu.VMEM((span, lanes), F32),
            pltpu.VMEM((lanes, span), F32),
            pltpu.VMEM((all_hands, all_hands), BF16),
            pltpu.VMEM((all_hands, all_hands), BF16),
            pltpu.VMEM((count, all_hands), F32),
            pltpu.VMEM((chunks, hands, 8, width), jnp.int16),
            pltpu.VMEM((chunks, leafs * hands, 8, width), jnp.int16),
            pltpu.VMEM((chunks, 1, 128), F32),
            pltpu.VMEM((chunks, leafs * hands, 1, 128), F32),
            dma(()), dma((max(leafs // 2, 1),)), dma(()), dma(()), dma(()),
            dma(()), dma((chunks,)), dma(()), dma(()), dma(()), dma(()),
            dma(()), dma((chunks,)), dma(()), dma((chunks,)),
            dma((chunks,)), dma((2,)),
        ],
        compiler_params=pltpu.CompilerParams(
            collective_id=0, has_side_effects=True, vmem_limit_bytes=VMEM_LIMIT
        ),
        name="evaluate",
    )(
        upper, parents, roots, boards, opp_range, br_range, cards, opp_actions, kinds, stakes,
        br_actions, ranks, weights,
    )
    return pl.pallas_call(
        spread_kernel,
        out_shape=(
            jax.ShapeDtypeStruct((levels, nodes_dev, width), F32),
            jax.ShapeDtypeStruct((width,), F32),
            jax.ShapeDtypeStruct((1, 1), F32),
        ),
        in_specs=[vmem()],
        out_specs=(vmem(), vmem(), pl.BlockSpec(memory_space=pltpu.SMEM)),
        name="spread",
    )(flat)


def local(
    opp_range,
    br_range,
    up_weight,
    up_parent,
    board_cards,
    hand_rank,
    root_parent,
    br_actions,
    opp_actions,
    leaf_kind,
    leaf_stake,
    opp_weight,
):
    hands_dev = up_weight.shape[2]
    boards_dev, hands_all = hand_rank.shape
    actions = opp_actions.shape[1]
    span = actions * actions
    leafs = lax.axis_size("leaf")
    hands = lax.axis_size("hand")
    cards = jnp.asarray(hand_cards(hands_all))
    boards = board_cards.T
    level_values, root, best = evaluate(
        up_weight,
        up_parent,
        root_parent[None, :],
        boards,
        opp_range[None, :],
        br_range[None, :],
        cards,
        opp_actions.T,
        leaf_kind.transpose(1, 2, 0).reshape(span, boards_dev),
        leaf_stake.transpose(1, 2, 0).reshape(span, boards_dev),
        br_actions,
        hand_rank,
        opp_weight.reshape(boards_dev, span, hands_dev),
        leafs,
        hands,
        actions,
    )
    return (level_values, root, best[0, 0])


def solution(mesh):
    in_specs = (
        P("hand"),
        P("hand"),
        P(None, "leaf", "hand"),
        P(),
        P("leaf", None),
        P("leaf", None),
        P("leaf"),
        P("leaf"),
        P("leaf", None),
        P("leaf", None, None),
        P("leaf", None, None),
        P("leaf", None, None, "hand"),
    )
    out_specs = (P(None, "leaf", "hand"), P("hand"), P())
    return jax.shard_map(local, mesh=mesh, in_specs=in_specs, out_specs=out_specs, check_vma=False)
```

```python
import functools

import jax
import jax.numpy as jnp
import numpy as np
from jax import lax
from jax.experimental import pallas as pl
from jax.experimental.pallas import tpu as pltpu
from jax.sharding import PartitionSpec as P

PAYOFF_UNIT = 1.0 / 4096.0
VMEM_LIMIT = 60 * 1024 * 1024
F32 = jnp.float32
BF16 = jnp.bfloat16
F8 = jnp.float8_e4m3fn


def hand_cards(number):
    low_list = []
    high_list = []
    for low_card in range(52):
        for high_card in range(low_card + 1, 52):
            low_list.append(low_card)
            high_list.append(high_card)
    chosen = np.arange(number) * 1326 // number
    cards = np.zeros((8, number), np.float32)
    cards[0] = np.array(low_list)[chosen]
    cards[1] = np.array(high_list)[chosen]
    cards[2] = np.exp2(np.arange(number) * 0.6180339887498949 % 1.0)
    cards[3] = 1.0 / cards[2]
    return cards


def vmem():
    return pl.BlockSpec(memory_space=pltpu.VMEM)


def hbm():
    return pl.BlockSpec(memory_space=pl.ANY)


def greet(axes_sizes):
    barrier = pltpu.get_barrier_semaphore()
    count = 0
    for axis, size in axes_sizes:
        me = lax.axis_index(axis)
        for dist in range(1, size):
            pl.semaphore_signal(
                barrier,
                inc=1,
                device_id={axis: lax.rem(me + dist, size)},
                device_id_type=pl.DeviceIdType.MESH,
            )
            count += 1
    pl.semaphore_wait(barrier, count)


def flip(index, mask):
    out = index
    bit = 1
    while bit <= mask:
        if mask & bit:
            out = out + bit - 2 * bit * lax.rem(index // bit, 2)
        bit *= 2
    return out


def peers_of(me, size):
    if size & (size - 1):
        return [lax.rem(me + dist, size) for dist in range(1, size)]
    far = [mask for mask in range(1, size) if mask >= size // 2]
    near = [mask for mask in range(1, size) if mask < size // 2]
    return [flip(me, mask) for mask in far + near]


def push(axis, peers, source, target, sem):
    for peer in peers:
        send(axis, peer, source(peer), target, sem).start()


def send(axis, peer, source, target, sem):
    send_sem, recv_sem = sem
    return pltpu.make_async_remote_copy(
        src_ref=source,
        dst_ref=target,
        send_sem=send_sem,
        recv_sem=recv_sem,
        device_id={axis: peer},
        device_id_type=pl.DeviceIdType.MESH,
    )


def settle(ref, sem):
    pltpu.make_async_copy(ref, ref, sem).wait()


def columns_of(ref, pad_ref):
    lines, count = ref.shape
    pad_ref[...] = jnp.zeros(pad_ref.shape, F32)
    pad_ref[0:lines, 0:count] = ref[...].astype(F32)
    return pad_ref[...].T


def kernel(
    leafs, hands, levels, actions,
    upper_ref, parent_ref, root_ref, board_ref, range_ref, br_ref, cards_ref, opp_ref, kind_ref, stake_ref,
    actions_ref, rank_ref, weight_ref,
    flat_out,
    every, weights, ranks_in, ratio, ratio_in, reach, reach_in, anc, anc_all, br_all,
    pad, board_columns, stake_lines, stake_rows, apart_ref, against_ref, apart_small, order_ref, scaled,
    ready, values_all, units, units_all,
    up_s, up_r, pass_r, anc_s, anc_r, ratio_s, ratio_r, reach_s, reach_r, br_s, br_r,
    value_s, value_r, unit_s, unit_r, load_sem, own_sem,
):
    leaf = lax.axis_index("leaf")
    hand = lax.axis_index("hand")
    count = ratio.shape[1] // (2 * actions)
    width = weights.shape[3]
    boards = hands * count
    chunks = count // 8
    all_hands = hands * width
    span = actions * actions
    both = 2 * actions
    nodes_dev = upper_ref.shape[1]
    nodes = leafs * nodes_dev
    partners = peers_of(hand, hands)
    others = [lax.rem(leaf + dist, leafs) for dist in range(1, leafs)]

    def load(part, chunk):
        first = pl.multiple_of(part * count + chunk * 8, 8)
        return pltpu.make_async_copy(
            weight_ref.at[pl.ds(first, 8)], weights.at[part, pl.ds(chunk * 8, 8)], load_sem.at[chunk]
        )

    parts = partners + [hand]
    for chunk in range(chunks):
        for part in parts:
            load(part, chunk).start()
    own_upper = pltpu.make_async_copy(upper_ref, every.at[leaf], own_sem.at[0])
    own_upper.start()
    own_ranks = pltpu.make_async_copy(
        rank_ref.at[pl.ds(pl.multiple_of(hand * count, 8), count)], ranks_in, own_sem.at[1]
    )
    own_ranks.start()
    greet((("leaf", leafs), ("hand", hands)))
    ring = leafs // 2
    side = lax.rem(leaf, 2)
    twin = leaf + 1 - 2 * side

    def up_copy(source, owner, peer, k):
        return pltpu.make_async_remote_copy(
            src_ref=source,
            dst_ref=every.at[owner],
            send_sem=up_s,
            recv_sem=pass_r if k is None else up_r.at[k],
            device_id={"leaf": peer},
            device_id_type=pl.DeviceIdType.MESH,
        )

    def around(dist):
        return lax.rem(leaf // 2 + dist, ring) * 2 + side

    steps = sorted(range(1, ring), key=lambda dist: min(dist, ring - dist))
    up_direct = {dist: up_copy(upper_ref, leaf, around(dist), dist) for dist in steps}
    up_direct[0] = up_copy(upper_ref, leaf, twin, 0)
    for dist in steps + [0]:
        up_direct[dist].start()

    def pass_on(dists):
        for dist in dists:
            up_direct[dist].wait_recv()
            origin = around(ring - dist)
            up_copy(every.at[origin], origin, twin, None).start()

    stake_lines[...] = jnp.zeros(stake_lines.shape, F32)
    reply_ids = lax.broadcasted_iota(jnp.int32, (actions, boards), 0)
    for a in range(actions):
        lines = slice(a * actions, (a + 1) * actions)
        stake = stake_ref[lines, :]
        signed = jnp.where(kind_ref[lines, :] == 1, stake, -stake)
        legal = reply_ids < opp_ref[a : a + 1, :]
        stake_lines[lines, 0:boards] = jnp.where(legal, signed, 0).astype(F32)
    stake_rows[...] = stake_lines[...].T

    diagonal = lax.broadcasted_iota(jnp.int32, (actions, span), 0) == (
        lax.broadcasted_iota(jnp.int32, (actions, span), 1) // actions
    )
    own_lanes = pl.ds(pl.multiple_of(hand * width, width), width)
    spread = cards_ref[2:3, own_lanes]

    def fold(part, chunk, target):
        lines = stake_rows[pl.ds(pl.multiple_of(part * count + chunk * 8, 8), 8), :]
        for i in range(8):
            stake = jnp.broadcast_to(lines[i : i + 1, :], (actions, span))
            stake = jnp.where(diagonal, stake, 0.0)
            legal = jnp.where(stake != 0.0, 1.0, 0.0)
            shown = jnp.maximum(stake, 0.0)
            folds = jnp.maximum(-stake, 0.0)
            shown_hi = jnp.floor(shown * 0.5) * 2.0
            fold_hi = jnp.floor(folds * 0.5) * 2.0
            rows = jnp.concatenate([legal, shown_hi, shown - shown_hi, fold_hi, folds - fold_hi], axis=0)
            sums = jnp.dot(rows.astype(BF16), weights[part, chunk * 8 + i], preferred_element_type=F32)
            piece = [sums[j * actions : (j + 1) * actions] for j in range(5)]
            scale = spread / piece[0]
            pair = jnp.concatenate(
                [(piece[1] + piece[2]) * scale, (piece[3] + piece[4]) * scale], axis=0
            )
            place = (chunk * 8 + i) * both
            target[part, place : place + both, :] = pair.astype(BF16)

    for chunk in range(chunks):
        block = pl.ds(chunk * 8 * both, 8 * both)
        settle(weights.at[:, pl.ds(chunk * 8, 8)], load_sem.at[chunk])
        for part in partners:
            fold(part, chunk, ratio)
            send(
                "hand", part, ratio.at[part, block], ratio_in.at[hand, block], (ratio_s, ratio_r.at[chunk])
            ).start()
    push("hand", partners, lambda peer: br_ref, br_all.at[hand], (br_s, br_r))
    br_all[hand] = br_ref[...]

    node_column = lax.broadcasted_iota(jnp.int32, (nodes, boards), 0)
    pad[...] = jnp.zeros(pad.shape, F32)
    line = root_ref[...]
    pad[levels - 1 : levels, 0:boards] = line.astype(F32)
    for level in range(levels - 2, -1, -1):
        parents = jnp.broadcast_to(parent_ref[level : level + 1, :], (8, nodes)).astype(F32)
        column = parents.T[:, 0:1]
        line_f = jnp.sum(jnp.where(node_column == line, column, 0.0), axis=0, keepdims=True)
        pad[level : level + 1, 0:boards] = line_f
        line = line_f.astype(jnp.int32)
    anc_float = pad[...].T
    anc_columns = anc_float.astype(jnp.int32)
    lane = lax.broadcasted_iota(jnp.int32, (boards, boards), 1)
    held = (lane % (hands * 8)) // 8 * count + lane // (hands * 8) * 8 + lane % 8
    moved = lax.broadcasted_iota(jnp.int32, (boards, boards), 0) == held
    anc[...] = jnp.zeros(anc.shape, F32)
    for level in range(levels):
        anc[level : level + 1, 0:boards] = jnp.sum(
            jnp.where(moved, anc_float[0:boards, level : level + 1], 0.0), axis=0, keepdims=True
        )
    push("leaf", others, lambda peer: anc, anc_all.at[leaf], (anc_s, anc_r))
    anc_all[leaf] = anc[...]

    low = cards_ref[0:1, :]
    high = cards_ref[1:2, :]
    card_columns = cards_ref[...].T
    deck_lanes = lax.broadcasted_iota(jnp.int32, (width, 128), 1).astype(F32)
    deck_rows = lax.broadcasted_iota(jnp.int32, (128, all_hands), 0).astype(F32)
    holds = jnp.where((deck_rows == low) | (deck_rows == high), 1.0, 0.0).astype(BF16)
    for part in range(hands):
        rows = slice(part * width, (part + 1) * width)
        held = (deck_lanes == card_columns[rows, 0:1]) | (deck_lanes == card_columns[rows, 1:2])
        held = jnp.where(held, 1.0, 0.0).astype(BF16)
        common = jnp.dot(held, holds, preferred_element_type=F32).astype(BF16)
        apart = jnp.maximum(1.0 - common, 0.0)
        apart_ref[rows, :] = apart
        against_ref[rows, :] = jnp.minimum(common - 1.0, 0.0)
        apart_small[rows, :] = apart.astype(F8)

    own_ranks.wait()
    ranks = ((ranks_in[...] % 128) + 128).astype(F32)
    octave = ranks_in[...] // 128
    for bit in (1, 2, 4, 8, 16, 32):
        ranks = ranks * jnp.where(octave // bit % 2 == 1, float(2**bit), 1.0)
    scaled[...] = ranks

    def compare(chunk, strips):
        rank_rows = scaled[pl.ds(pl.multiple_of(chunk * 8, 8), 8), :]
        rank_columns = rank_rows.T.astype(BF16)
        rank_rows = rank_rows.astype(BF16)
        for first in strips:
            lanes_of = slice(first, first + width)
            across = [jnp.broadcast_to(rank_rows[i : i + 1, lanes_of], (32, width)) for i in range(8)]
            for top in range(0, all_hands, 32):
                rows = slice(top, top + 32)
                against = against_ref[rows, lanes_of]
                apart = apart_ref[rows, lanes_of]
                for i in range(8):
                    sign = across[i] - rank_columns[rows, i : i + 1]
                    sign = jnp.minimum(jnp.maximum(sign, against), apart)
                    order_ref[chunk * 8 + i, rows, lanes_of] = sign.astype(F8)

    outer = [dist for dist in steps if dist in (1, ring - 1)]
    inner = [dist for dist in steps if dist not in (1, ring - 1)]
    parity = lax.rem(hand, 2)

    def pass_if(which, dists):
        @pl.when(parity == which)
        def _():
            pass_on(dists)

    strips = list(range(0, all_hands, width))
    half = len(strips) // 2
    pass_if(1, outer)
    compare(0, strips[:half])
    pass_if(1, inner)
    compare(0, strips[half:])
    pass_if(0, outer)
    early = min(chunks, 2)
    for chunk in range(1, early):
        compare(chunk, strips[:half])
    pass_if(0, inner)
    for chunk in range(1, early):
        compare(chunk, strips[half:])
    for chunk in range(chunks):
        fold(hand, chunk, ratio_in)

    own_low = cards_ref[0:1, own_lanes]
    own_high = cards_ref[1:2, own_lanes]
    board_columns[...] = columns_of(board_ref, pad)
    free = jnp.ones((boards, width), F32)
    for card in range(5):
        column = board_columns[0:boards, card : card + 1]
        free = jnp.where((column == own_low) | (column == own_high), 0.0, free)
    free = free * cards_ref[3:4, own_lanes]

    own_upper.wait()
    up_direct[0].wait_recv()
    settle(every.at[pl.ds(0, ring - 1)], pass_r)
    settle(every.at[pl.ds(0, leafs - 1)], up_s)
    node_ids = lax.broadcasted_iota(jnp.int32, (boards, nodes), 1)
    total = jnp.broadcast_to(range_ref[...], (boards, width))
    for level in range(levels):
        pick = jnp.where(anc_columns[0:boards, level : level + 1] == node_ids, 1.0, 0.0).astype(BF16)
        table = every[:, level].reshape(nodes, width)
        total = total * jnp.dot(pick, table, preferred_element_type=F32)
    total = total * free
    for part in range(hands):
        for chunk in range(chunks):
            first = part * count + chunk * 8
            reach[part, chunk] = total[first : first + 8].astype(BF16)
    push("hand", partners, lambda peer: reach.at[peer], reach_in.at[hand], (reach_s, reach_r))
    reach_in[hand] = reach[hand]
    action_ids = lax.broadcasted_iota(jnp.int32, (actions, 1), 0)
    settle(br_all.at[pl.ds(0, hands - 1)], br_r)
    br_row = jnp.concatenate([br_all[part] for part in range(hands)], axis=1)

    def partial(chunk, group):
        lines = []
        folded = jnp.zeros((8 * both, all_hands), F32)
        for part in group:
            rows = slice(part * width, (part + 1) * width)
            pieces = []
            reach_rows = reach_in[part, chunk].astype(F32)
            for i in range(8):
                b = chunk * 8 + i
                row = ratio_in[part, pl.ds(pl.multiple_of(b * both, both), both), :].astype(F32)
                pieces.append((row * reach_rows[i : i + 1, :]).astype(BF16))
            lines.append((rows, pieces))
            folded = folded + jnp.dot(
                jnp.concatenate(pieces, axis=0), apart_small[rows, :], preferred_element_type=F32
            )
        nodes_of = []
        for i in range(8):
            shown = jnp.zeros((both, all_hands), F32)
            for rows, pieces in lines:
                shown = shown + jnp.dot(
                    pieces[i], order_ref[chunk * 8 + i, rows, :], preferred_element_type=F32
                )
            nodes_of.append(shown[0:actions] + folded[i * both + actions : (i + 1) * both])
        return nodes_of

    def finish(chunk, nodes_of):
        first = pl.multiple_of(hand * count + chunk * 8, 8)
        cards_on = board_columns[pl.ds(first, 8), :]
        open_hands = jnp.ones((8, all_hands), F32)
        for card in range(5):
            column = cards_on[:, card : card + 1]
            open_hands = jnp.where((column == low) | (column == high), 0.0, open_hands)
        best_rows = []
        for i in range(8):
            allowed = action_ids < actions_ref[first + i]
            best_rows.append(jnp.max(jnp.where(allowed, nodes_of[i], -1e30), axis=0, keepdims=True))
        best = jnp.concatenate(best_rows, axis=0) * (open_hands * PAYOFF_UNIT)
        peak = jnp.max(jnp.abs(best), axis=1, keepdims=True) * (1.0 / 32640.0)
        unit = jnp.full((8, 1), 2.0**16, F32)
        inverse = jnp.full((8, 1), 2.0**-16, F32)
        for bit in (64, 32, 16, 8, 4, 2, 1):
            fits = peak <= unit * 2.0**-bit
            unit = jnp.where(fits, unit * 2.0**-bit, unit)
            inverse = jnp.where(fits, inverse * 2.0**bit, inverse)
        codes = jnp.floor(best * inverse + 0.5).astype(jnp.int32).astype(jnp.int16)
        for part in range(hands):
            ready[chunk, part] = codes[:, part * width : (part + 1) * width]
        share = jnp.sum(jnp.sum(best * br_row, axis=1, keepdims=True), axis=0, keepdims=True)
        lane = lax.broadcasted_iota(jnp.int32, (8, 128), 1)
        place = hand * 8 + lax.broadcasted_iota(jnp.int32, (8, 128), 0)
        row = jnp.sum(jnp.where(lane == place, unit, 0.0), axis=0, keepdims=True)
        units[chunk] = jnp.where(lane[0:1] == hands * 8, share, row)

    peers = leafs * hands

    behind = len(inner) * hands

    def ship(chunk, what, slots, target, sem_set):
        for kind, source, place in what:
            pltpu.make_async_remote_copy(
                src_ref=source,
                dst_ref=place.at[chunk, slots],
                send_sem=(value_s, unit_s)[kind],
                recv_sem=(value_r, unit_r)[kind].at[sem_set, chunk],
                device_id=target,
                device_id_type=pl.DeviceIdType.MESH,
            ).start()

    def send_chunk(chunk, direct):
        own = leaf * hands + hand
        for dist in range(ring):
            for cross in (0, 1):
                if cross and dist in inner and not direct:
                    continue
                to_leaf = around(dist)
                if cross:
                    to_leaf = to_leaf + 1 - 2 * side
                group = 1 if dist in inner and not direct else 0
                for dh in range(hands):
                    if dist == 0 and not cross and dh == 0:
                        continue
                    to_hand = lax.rem(hand + dh, hands)
                    what = [(0, ready.at[chunk, to_hand], values_all), (1, units.at[chunk], units_all)]
                    ship(chunk, what, own, {"leaf": to_leaf, "hand": to_hand}, group)
        values_all[chunk, own] = ready[chunk, hand]
        units_all[chunk, own] = units[chunk]

    def collect(chunk, blocks, sem_set):
        if blocks:
            settle(values_all.at[chunk, pl.ds(0, blocks)], value_r.at[sem_set, chunk])
            settle(units_all.at[chunk, pl.ds(0, blocks)], unit_r.at[sem_set, chunk])

    def relay_chunk(chunk):
        collect(chunk, behind, 1)
        for dist in inner:
            slots = pl.ds(around(dist) * hands, hands)
            what = [(0, values_all.at[chunk, slots], values_all), (1, units_all.at[chunk, slots], units_all)]
            ship(chunk, what, slots, {"leaf": twin}, 2)

    def one_chunk(chunk, carry):
        finish(chunk, partial(chunk, list(range(hands))))
        send_chunk(chunk, False)
        return carry

    for chunk in range(early, chunks):
        compare(chunk, strips)
    for chunk in range(chunks):
        settle(ratio.at[pl.ds(0, hands - 1), pl.ds(0, 8 * both)], ratio_r.at[chunk])
    settle(reach.at[pl.ds(0, hands - 1)], reach_r)
    lax.fori_loop(0, chunks - 1, one_chunk, 0)
    finish(chunks - 1, partial(chunks - 1, list(range(hands))))
    send_chunk(chunks - 1, True)
    for chunk in range(chunks - 1):
        relay_chunk(chunk)
    settle(ratio.at[pl.ds(0, hands - 1)], ratio_s)
    settle(reach.at[pl.ds(0, hands - 1)], reach_s)
    settle(br_all.at[pl.ds(0, hands - 1)], br_s)

    settle(anc_all.at[pl.ds(0, leafs - 1)], anc_r)
    settle(anc_all.at[pl.ds(0, leafs - 1)], anc_s)
    lines_dev = levels * nodes_dev
    block = hands * 8
    together = max(width // block, 1)
    groups = [list(range(k, min(k + together, leafs))) for k in range(0, leafs, together)]

    def add_group(chunk, group, sums):
        own = pl.ds(group[0] * hands, len(group) * hands)
        tall = len(group) * block
        lines = [anc_all[source][:, chunk * block : (chunk + 1) * block] for source in group]
        lines = jnp.concatenate(lines, axis=1)
        node_rows = leaf * nodes_dev + lax.broadcasted_iota(jnp.int32, (nodes_dev, tall), 0)
        node_rows = node_rows.astype(F32)
        rows = [
            jnp.sum(units_all[chunk, source * hands : (source + 1) * hands], axis=0) for source in group
        ]
        unit = jnp.concatenate([row[:, 0:block] for row in rows], axis=1)
        part = values_all[chunk, own].astype(jnp.int32).astype(F32).reshape(tall, width)
        coarse = part.astype(BF16)
        fine = (part - coarse.astype(F32)).astype(BF16)
        pick = [jnp.where(lines[k : k + 1, :] == node_rows, unit, 0.0) for k in range(levels)]
        pick = jnp.concatenate(pick + [jnp.broadcast_to(unit, (8, tall))], axis=0).astype(BF16)
        sums = sums + jnp.dot(pick, coarse, preferred_element_type=F32)
        share = sum(row[:, block : block + 1] for row in rows)
        return sums + jnp.dot(pick, fine, preferred_element_type=F32), share

    sums = jnp.zeros((lines_dev + 8, width), F32)
    whole = jnp.zeros((1, 1), F32)
    for chunk in range(chunks):
        if chunk < chunks - 1:
            collect(chunk, peers - 1 - 2 * behind, 0)
            collect(chunk, behind, 2)
        else:
            collect(chunk, peers - 1, 0)
        for group in groups:
            sums, share = add_group(chunk, group, sums)
            whole = whole + share
    flat_out[0:lines_dev] = sums[0:lines_dev]
    for chunk in range(chunks):
        settle(values_all.at[chunk, pl.ds(0, peers - 1)], value_s)
        settle(units_all.at[chunk, pl.ds(0, peers - 1)], unit_s)
    best = whole / nodes / jnp.sum(br_row, axis=1, keepdims=True)
    line = lax.broadcasted_iota(jnp.int32, (8, width), 0)
    flat_out[lines_dev:] = jnp.where(line == 0, sums[lines_dev:] / nodes, best)


def spread_kernel(flat_ref, level_out, root_out, best_out):
    levels, nodes_dev, _ = level_out.shape
    for k in range(levels):
        level_out[k] = flat_ref[k * nodes_dev : (k + 1) * nodes_dev]
    root_out[...] = flat_ref[levels * nodes_dev]
    best_out[0, 0] = flat_ref[levels * nodes_dev + 1, 0]


def evaluate(
    upper, parents, roots, boards, opp_range, br_range, cards, opp_actions, kinds, stakes,
    br_actions, ranks, weights, leafs, hands, actions,
):
    levels, nodes_dev, width = upper.shape
    boards_dev, span, _ = weights.shape
    count = boards_dev // hands
    chunks = count // 8
    both = 2 * actions
    all_hands = ranks.shape[1]
    lanes = -(-boards_dev // 128) * 128
    dma = pltpu.SemaphoreType.DMA
    flat = pl.pallas_call(
        functools.partial(kernel, leafs, hands, levels, actions),
        out_shape=jax.ShapeDtypeStruct((levels * nodes_dev + 8, width), F32),
        in_specs=[vmem()] * 10 + [pl.BlockSpec(memory_space=pltpu.SMEM), hbm(), hbm()],
        out_specs=vmem(),
        scratch_shapes=[
            pltpu.VMEM((leafs, levels, nodes_dev, width), BF16),
            pltpu.VMEM((hands, count, span, width), BF16),
            pltpu.VMEM((count, all_hands), jnp.int32),
            pltpu.VMEM((hands, count * both, width), BF16),
            pltpu.VMEM((hands, count * both, width), BF16),
            pltpu.VMEM((hands, chunks, 8, width), BF16),
            pltpu.VMEM((hands, chunks, 8, width), BF16),
            pltpu.VMEM((8, lanes), F32),
            pltpu.VMEM((leafs, 8, lanes), F32),
            pltpu.VMEM((hands, 1, width), F32),
            pltpu.VMEM((8, lanes), F32),
            pltpu.VMEM((lanes, 8), F32),
            pltpu.VMEM((span, lanes), F32),
            pltpu.VMEM((lanes, span), F32),
            pltpu.VMEM((all_hands, all_hands), BF16),
            pltpu.VMEM((all_hands, all_hands), BF16),
            pltpu.VMEM((all_hands, all_hands), F8),
            pltpu.VMEM((count, all_hands, all_hands), F8),
            pltpu.VMEM((count, all_hands), F32),
            pltpu.VMEM((chunks, hands, 8, width), jnp.int16),
            pltpu.VMEM((chunks, leafs * hands, 8, width), jnp.int16),
            pltpu.VMEM((chunks, 1, 128), F32),
            pltpu.VMEM((chunks, leafs * hands, 1, 128), F32),
            dma(()), dma((max(leafs // 2, 1),)), dma(()), dma(()), dma(()),
            dma(()), dma((chunks,)), dma(()), dma(()), dma(()), dma(()),
            dma(()), dma((3, chunks)), dma(()), dma((3, chunks)),
            dma((chunks,)), dma((2,)),
        ],
        compiler_params=pltpu.CompilerParams(
            collective_id=0, has_side_effects=True, vmem_limit_bytes=VMEM_LIMIT
        ),
        name="evaluate",
    )(
        upper, parents, roots, boards, opp_range, br_range, cards, opp_actions, kinds, stakes,
        br_actions, ranks, weights,
    )
    return pl.pallas_call(
        spread_kernel,
        out_shape=(
            jax.ShapeDtypeStruct((levels, nodes_dev, width), F32),
            jax.ShapeDtypeStruct((width,), F32),
            jax.ShapeDtypeStruct((1, 1), F32),
        ),
        in_specs=[vmem()],
        out_specs=(vmem(), vmem(), pl.BlockSpec(memory_space=pltpu.SMEM)),
        name="spread",
    )(flat)


def local(
    opp_range,
    br_range,
    up_weight,
    up_parent,
    board_cards,
    hand_rank,
    root_parent,
    br_actions,
    opp_actions,
    leaf_kind,
    leaf_stake,
    opp_weight,
):
    hands_dev = up_weight.shape[2]
    boards_dev, hands_all = hand_rank.shape
    actions = opp_actions.shape[1]
    span = actions * actions
    leafs = lax.axis_size("leaf")
    hands = lax.axis_size("hand")
    cards = jnp.asarray(hand_cards(hands_all))
    boards = board_cards.T
    level_values, root, best = evaluate(
        up_weight,
        up_parent,
        root_parent[None, :],
        boards,
        opp_range[None, :],
        br_range[None, :],
        cards,
        opp_actions.T,
        leaf_kind.transpose(1, 2, 0).reshape(span, boards_dev),
        leaf_stake.transpose(1, 2, 0).reshape(span, boards_dev),
        br_actions,
        hand_rank,
        opp_weight.reshape(boards_dev, span, hands_dev),
        leafs,
        hands,
        actions,
    )
    return (level_values, root, best[0, 0])


def solution(mesh):
    in_specs = (
        P("hand"),
        P("hand"),
        P(None, "leaf", "hand"),
        P(),
        P("leaf", None),
        P("leaf", None),
        P("leaf"),
        P("leaf"),
        P("leaf", None),
        P("leaf", None, None),
        P("leaf", None, None),
        P("leaf", None, None, "hand"),
    )
    out_specs = (P(None, "leaf", "hand"), P("hand"), P())
    return jax.shard_map(local, mesh=mesh, in_specs=in_specs, out_specs=out_specs, check_vma=False)
```

```python
import functools

import jax
import jax.numpy as jnp
import numpy as np
from jax import lax
from jax.experimental import pallas as pl
from jax.experimental.pallas import tpu as pltpu
from jax.sharding import PartitionSpec as P

PAYOFF_UNIT = 1.0 / 4096.0
VMEM_LIMIT = 60 * 1024 * 1024
F32 = jnp.float32
BF16 = jnp.bfloat16
F8 = jnp.float8_e4m3fn


def hand_cards(number):
    low_list = []
    high_list = []
    for low_card in range(52):
        for high_card in range(low_card + 1, 52):
            low_list.append(low_card)
            high_list.append(high_card)
    chosen = np.arange(number) * 1326 // number
    cards = np.zeros((8, number), np.float32)
    cards[0] = np.array(low_list)[chosen]
    cards[1] = np.array(high_list)[chosen]
    cards[2] = np.exp2(np.arange(number) * 0.6180339887498949 % 1.0)
    cards[3] = 1.0 / cards[2]
    return cards


def vmem():
    return pl.BlockSpec(memory_space=pltpu.VMEM)


def hbm():
    return pl.BlockSpec(memory_space=pl.ANY)


def greet(axes_sizes):
    barrier = pltpu.get_barrier_semaphore()
    count = 0
    for axis, size in axes_sizes:
        me = lax.axis_index(axis)
        for dist in range(1, size):
            pl.semaphore_signal(
                barrier,
                inc=1,
                device_id={axis: lax.rem(me + dist, size)},
                device_id_type=pl.DeviceIdType.MESH,
            )
            count += 1
    pl.semaphore_wait(barrier, count)


def flip(index, mask):
    out = index
    bit = 1
    while bit <= mask:
        if mask & bit:
            out = out + bit - 2 * bit * lax.rem(index // bit, 2)
        bit *= 2
    return out


def peers_of(me, size):
    if size & (size - 1):
        return [lax.rem(me + dist, size) for dist in range(1, size)]
    far = [mask for mask in range(1, size) if mask >= size // 2]
    near = [mask for mask in range(1, size) if mask < size // 2]
    return [flip(me, mask) for mask in far + near]


def push(axis, peers, source, target, sem):
    for peer in peers:
        send(axis, peer, source(peer), target, sem).start()


def send(axis, peer, source, target, sem):
    send_sem, recv_sem = sem
    return pltpu.make_async_remote_copy(
        src_ref=source,
        dst_ref=target,
        send_sem=send_sem,
        recv_sem=recv_sem,
        device_id={axis: peer},
        device_id_type=pl.DeviceIdType.MESH,
    )


def settle(ref, sem):
    pltpu.make_async_copy(ref, ref, sem).wait()


def columns_of(ref, pad_ref):
    lines, count = ref.shape
    pad_ref[...] = jnp.zeros(pad_ref.shape, F32)
    pad_ref[0:lines, 0:count] = ref[...].astype(F32)
    return pad_ref[...].T


def kernel(
    leafs, hands, levels, actions,
    upper_ref, parent_ref, root_ref, board_ref, range_ref, br_ref, cards_ref, opp_ref, kind_ref, stake_ref,
    actions_ref, rank_ref, weight_ref,
    flat_out,
    every, weights, ranks_in, ratio, ratio_in, reach, reach_in, anc, anc_all, br_all,
    pad, board_columns, stake_lines, stake_rows, apart_ref, against_ref, apart_small, order_ref, scaled,
    ready, values_all, units, units_all,
    up_s, up_r, pass_r, anc_s, anc_r, ratio_s, ratio_r, reach_s, reach_r, br_s, br_r,
    value_s, value_r, unit_s, unit_r, load_sem, own_sem,
):
    leaf = lax.axis_index("leaf")
    hand = lax.axis_index("hand")
    count = ratio.shape[1] // (2 * actions)
    width = weights.shape[3]
    boards = hands * count
    chunks = count // 8
    all_hands = hands * width
    span = actions * actions
    both = 2 * actions
    nodes_dev = upper_ref.shape[1]
    nodes = leafs * nodes_dev
    partners = peers_of(hand, hands)
    others = [lax.rem(leaf + dist, leafs) for dist in range(1, leafs)]

    def load(part, chunk):
        first = pl.multiple_of(part * count + chunk * 8, 8)
        return pltpu.make_async_copy(
            weight_ref.at[pl.ds(first, 8)], weights.at[part, pl.ds(chunk * 8, 8)], load_sem.at[chunk]
        )

    parts = partners + [hand]
    for chunk in range(chunks):
        for part in parts:
            load(part, chunk).start()
    own_upper = pltpu.make_async_copy(upper_ref, every.at[leaf], own_sem.at[0])
    own_upper.start()
    own_ranks = pltpu.make_async_copy(
        rank_ref.at[pl.ds(pl.multiple_of(hand * count, 8), count)], ranks_in, own_sem.at[1]
    )
    own_ranks.start()
    greet((("leaf", leafs), ("hand", hands)))
    ring = leafs // 2
    side = lax.rem(leaf, 2)
    twin = leaf + 1 - 2 * side

    def up_copy(source, owner, peer, k):
        return pltpu.make_async_remote_copy(
            src_ref=source,
            dst_ref=every.at[owner],
            send_sem=up_s,
            recv_sem=pass_r if k is None else up_r.at[k],
            device_id={"leaf": peer},
            device_id_type=pl.DeviceIdType.MESH,
        )

    def around(dist):
        return lax.rem(leaf // 2 + dist, ring) * 2 + side

    steps = sorted(range(1, ring), key=lambda dist: min(dist, ring - dist))
    up_direct = {dist: up_copy(upper_ref, leaf, around(dist), dist) for dist in steps}
    up_direct[0] = up_copy(upper_ref, leaf, twin, 0)
    for dist in steps + [0]:
        up_direct[dist].start()

    def pass_on(dists):
        for dist in dists:
            up_direct[dist].wait_recv()
            origin = around(ring - dist)
            up_copy(every.at[origin], origin, twin, None).start()

    stake_lines[...] = jnp.zeros(stake_lines.shape, F32)
    reply_ids = lax.broadcasted_iota(jnp.int32, (actions, boards), 0)
    for a in range(actions):
        lines = slice(a * actions, (a + 1) * actions)
        stake = stake_ref[lines, :]
        signed = jnp.where(kind_ref[lines, :] == 1, stake, -stake)
        legal = reply_ids < opp_ref[a : a + 1, :]
        stake_lines[lines, 0:boards] = jnp.where(legal, signed, 0).astype(F32)
    stake_rows[...] = stake_lines[...].T

    diagonal = lax.broadcasted_iota(jnp.int32, (actions, span), 0) == (
        lax.broadcasted_iota(jnp.int32, (actions, span), 1) // actions
    )
    own_lanes = pl.ds(pl.multiple_of(hand * width, width), width)
    spread = cards_ref[2:3, own_lanes]

    def fold(part, chunk, target):
        lines = stake_rows[pl.ds(pl.multiple_of(part * count + chunk * 8, 8), 8), :]
        for i in range(8):
            stake = jnp.broadcast_to(lines[i : i + 1, :], (actions, span))
            stake = jnp.where(diagonal, stake, 0.0)
            legal = jnp.where(stake != 0.0, 1.0, 0.0)
            shown = jnp.maximum(stake, 0.0)
            folds = jnp.maximum(-stake, 0.0)
            shown_hi = jnp.floor(shown * 0.5) * 2.0
            fold_hi = jnp.floor(folds * 0.5) * 2.0
            rows = jnp.concatenate([legal, shown_hi, shown - shown_hi, fold_hi, folds - fold_hi], axis=0)
            sums = jnp.dot(rows.astype(BF16), weights[part, chunk * 8 + i], preferred_element_type=F32)
            piece = [sums[j * actions : (j + 1) * actions] for j in range(5)]
            scale = spread / piece[0]
            pair = jnp.concatenate(
                [(piece[1] + piece[2]) * scale, (piece[3] + piece[4]) * scale], axis=0
            )
            place = (chunk * 8 + i) * both
            target[part, place : place + both, :] = pair.astype(BF16)

    for chunk in range(chunks):
        block = pl.ds(chunk * 8 * both, 8 * both)
        settle(weights.at[:, pl.ds(chunk * 8, 8)], load_sem.at[chunk])
        for part in partners:
            fold(part, chunk, ratio)
            send(
                "hand", part, ratio.at[part, block], ratio_in.at[hand, block], (ratio_s, ratio_r.at[chunk])
            ).start()
    push("hand", partners, lambda peer: br_ref, br_all.at[hand], (br_s, br_r))
    br_all[hand] = br_ref[...]

    node_column = lax.broadcasted_iota(jnp.int32, (nodes, boards), 0)
    pad[...] = jnp.zeros(pad.shape, F32)
    line = root_ref[...]
    pad[levels - 1 : levels, 0:boards] = line.astype(F32)
    for level in range(levels - 2, -1, -1):
        parents = jnp.broadcast_to(parent_ref[level : level + 1, :], (8, nodes)).astype(F32)
        column = parents.T[:, 0:1]
        line_f = jnp.sum(jnp.where(node_column == line, column, 0.0), axis=0, keepdims=True)
        pad[level : level + 1, 0:boards] = line_f
        line = line_f.astype(jnp.int32)
    anc_float = pad[...].T
    anc_columns = anc_float.astype(jnp.int32)
    lane = lax.broadcasted_iota(jnp.int32, (boards, boards), 1)
    held = (lane % (hands * 8)) // 8 * count + lane // (hands * 8) * 8 + lane % 8
    moved = lax.broadcasted_iota(jnp.int32, (boards, boards), 0) == held
    anc[...] = jnp.zeros(anc.shape, F32)
    for level in range(levels):
        anc[level : level + 1, 0:boards] = jnp.sum(
            jnp.where(moved, anc_float[0:boards, level : level + 1], 0.0), axis=0, keepdims=True
        )
    push("leaf", others, lambda peer: anc, anc_all.at[leaf], (anc_s, anc_r))
    anc_all[leaf] = anc[...]

    low = cards_ref[0:1, :]
    high = cards_ref[1:2, :]
    card_columns = cards_ref[...].T
    deck_lanes = lax.broadcasted_iota(jnp.int32, (width, 128), 1).astype(F32)
    deck_rows = lax.broadcasted_iota(jnp.int32, (128, all_hands), 0).astype(F32)
    holds = jnp.where((deck_rows == low) | (deck_rows == high), 1.0, 0.0).astype(BF16)
    for part in range(hands):
        rows = slice(part * width, (part + 1) * width)
        held = (deck_lanes == card_columns[rows, 0:1]) | (deck_lanes == card_columns[rows, 1:2])
        held = jnp.where(held, 1.0, 0.0).astype(BF16)
        common = jnp.dot(held, holds, preferred_element_type=F32).astype(BF16)
        apart = jnp.maximum(1.0 - common, 0.0)
        apart_ref[rows, :] = apart
        against_ref[rows, :] = jnp.minimum(common - 1.0, 0.0)
        apart_small[rows, :] = apart.astype(F8)

    own_ranks.wait()
    ranks = ((ranks_in[...] % 128) + 128).astype(F32)
    octave = ranks_in[...] // 128
    for bit in (1, 2, 4, 8, 16, 32):
        ranks = ranks * jnp.where(octave // bit % 2 == 1, float(2**bit), 1.0)
    scaled[...] = ranks

    def compare(chunk, strips):
        rank_rows = scaled[pl.ds(pl.multiple_of(chunk * 8, 8), 8), :]
        rank_columns = rank_rows.T.astype(BF16)
        rank_rows = rank_rows.astype(BF16)
        for first in strips:
            lanes_of = slice(first, first + width)
            across = [jnp.broadcast_to(rank_rows[i : i + 1, lanes_of], (32, width)) for i in range(8)]
            for top in range(0, all_hands, 32):
                rows = slice(top, top + 32)
                against = against_ref[rows, lanes_of]
                apart = apart_ref[rows, lanes_of]
                for i in range(8):
                    sign = across[i] - rank_columns[rows, i : i + 1]
                    sign = jnp.minimum(jnp.maximum(sign, against), apart)
                    order_ref[chunk * 8 + i, rows, lanes_of] = sign.astype(F8)

    outer = [dist for dist in steps if dist in (1, ring - 1)]
    inner = [dist for dist in steps if dist not in (1, ring - 1)]
    parity = lax.rem(hand, 2)

    def pass_if(which, dists):
        @pl.when(parity == which)
        def _():
            pass_on(dists)

    strips = list(range(0, all_hands, width))
    half = len(strips) // 2
    pass_if(1, outer)
    compare(0, strips[:half])
    pass_if(1, inner)
    compare(0, strips[half:])
    pass_if(0, outer)
    early = min(chunks, 2)
    for chunk in range(1, early):
        compare(chunk, strips[:half])
    pass_if(0, inner)
    for chunk in range(1, early):
        compare(chunk, strips[half:])
    for chunk in range(chunks):
        fold(hand, chunk, ratio_in)

    own_low = cards_ref[0:1, own_lanes]
    own_high = cards_ref[1:2, own_lanes]
    board_columns[...] = columns_of(board_ref, pad)
    free = jnp.ones((boards, width), F32)
    for card in range(5):
        column = board_columns[0:boards, card : card + 1]
        free = jnp.where((column == own_low) | (column == own_high), 0.0, free)
    free = free * cards_ref[3:4, own_lanes]

    own_upper.wait()
    up_direct[0].wait_recv()
    settle(every.at[pl.ds(0, ring - 1)], pass_r)
    settle(every.at[pl.ds(0, leafs - 1)], up_s)
    node_ids = lax.broadcasted_iota(jnp.int32, (boards, nodes), 1)
    total = jnp.broadcast_to(range_ref[...], (boards, width))
    for level in range(levels):
        pick = jnp.where(anc_columns[0:boards, level : level + 1] == node_ids, 1.0, 0.0).astype(BF16)
        table = every[:, level].reshape(nodes, width)
        total = total * jnp.dot(pick, table, preferred_element_type=F32)
    total = total * free
    for part in range(hands):
        for chunk in range(chunks):
            first = part * count + chunk * 8
            reach[part, chunk] = total[first : first + 8].astype(BF16)
    push("hand", partners, lambda peer: reach.at[peer], reach_in.at[hand], (reach_s, reach_r))
    reach_in[hand] = reach[hand]
    action_ids = lax.broadcasted_iota(jnp.int32, (actions, 1), 0)
    settle(br_all.at[pl.ds(0, hands - 1)], br_r)
    br_row = jnp.concatenate([br_all[part] for part in range(hands)], axis=1)

    def partial(chunk, group):
        lines = []
        folded = jnp.zeros((8 * both, all_hands), F32)
        for part in group:
            rows = slice(part * width, (part + 1) * width)
            pieces = []
            reach_rows = reach_in[part, chunk].astype(F32)
            for i in range(8):
                b = chunk * 8 + i
                row = ratio_in[part, pl.ds(pl.multiple_of(b * both, both), both), :].astype(F32)
                pieces.append((row * reach_rows[i : i + 1, :]).astype(BF16))
            lines.append((rows, pieces))
            folded = folded + jnp.dot(
                jnp.concatenate(pieces, axis=0), apart_small[rows, :], preferred_element_type=F32
            )
        nodes_of = []
        for i in range(8):
            shown = jnp.zeros((both, all_hands), F32)
            for rows, pieces in lines:
                shown = shown + jnp.dot(
                    pieces[i], order_ref[chunk * 8 + i, rows, :], preferred_element_type=F32
                )
            nodes_of.append(shown[0:actions] + folded[i * both + actions : (i + 1) * both])
        return nodes_of

    def finish(chunk, nodes_of):
        first = pl.multiple_of(hand * count + chunk * 8, 8)
        cards_on = board_columns[pl.ds(first, 8), :]
        open_hands = jnp.ones((8, all_hands), F32)
        for card in range(5):
            column = cards_on[:, card : card + 1]
            open_hands = jnp.where((column == low) | (column == high), 0.0, open_hands)
        best_rows = []
        for i in range(8):
            allowed = action_ids < actions_ref[first + i]
            best_rows.append(jnp.max(jnp.where(allowed, nodes_of[i], -1e30), axis=0, keepdims=True))
        best = jnp.concatenate(best_rows, axis=0) * (open_hands * PAYOFF_UNIT)
        peak = jnp.max(jnp.abs(best), axis=1, keepdims=True) * (1.0 / 32640.0)
        unit = jnp.full((8, 1), 2.0**16, F32)
        inverse = jnp.full((8, 1), 2.0**-16, F32)
        for bit in (64, 32, 16, 8, 4, 2, 1):
            fits = peak <= unit * 2.0**-bit
            unit = jnp.where(fits, unit * 2.0**-bit, unit)
            inverse = jnp.where(fits, inverse * 2.0**bit, inverse)
        codes = jnp.floor(best * inverse + 0.5).astype(jnp.int32).astype(jnp.int16)
        for part in range(hands):
            ready[chunk, part] = codes[:, part * width : (part + 1) * width]
        share = jnp.sum(jnp.sum(best * br_row, axis=1, keepdims=True), axis=0, keepdims=True)
        lane = lax.broadcasted_iota(jnp.int32, (8, 128), 1)
        place = hand * 8 + lax.broadcasted_iota(jnp.int32, (8, 128), 0)
        row = jnp.sum(jnp.where(lane == place, unit, 0.0), axis=0, keepdims=True)
        units[chunk] = jnp.where(lane[0:1] == hands * 8, share, row)

    peers = leafs * hands

    behind = len(inner) * hands

    def ship(chunk, what, slots, target, sem_set):
        for kind, source, place in what:
            pltpu.make_async_remote_copy(
                src_ref=source,
                dst_ref=place.at[chunk, slots],
                send_sem=(value_s, unit_s)[kind],
                recv_sem=(value_r, unit_r)[kind].at[sem_set, chunk],
                device_id=target,
                device_id_type=pl.DeviceIdType.MESH,
            ).start()

    def send_chunk(chunk, direct):
        own = leaf * hands + hand
        for dist in inner + outer + [0]:
            for cross in (1, 0):
                if cross and dist in inner and not direct:
                    continue
                to_leaf = around(dist)
                if cross:
                    to_leaf = to_leaf + 1 - 2 * side
                group = 1 if dist in inner and not direct else 0
                for dh in range(hands):
                    if dist == 0 and not cross and dh == 0:
                        continue
                    to_hand = lax.rem(hand + dh, hands)
                    what = [(0, ready.at[chunk, to_hand], values_all), (1, units.at[chunk], units_all)]
                    ship(chunk, what, own, {"leaf": to_leaf, "hand": to_hand}, group)
        values_all[chunk, own] = ready[chunk, hand]
        units_all[chunk, own] = units[chunk]

    def collect(chunk, blocks, sem_set):
        if blocks:
            settle(values_all.at[chunk, pl.ds(0, blocks)], value_r.at[sem_set, chunk])
            settle(units_all.at[chunk, pl.ds(0, blocks)], unit_r.at[sem_set, chunk])

    def relay_chunk(chunk):
        collect(chunk, behind, 1)
        for dist in inner:
            slots = pl.ds(around(dist) * hands, hands)
            what = [(0, values_all.at[chunk, slots], values_all), (1, units_all.at[chunk, slots], units_all)]
            ship(chunk, what, slots, {"leaf": twin}, 2)

    def one_chunk(chunk, carry):
        finish(chunk, partial(chunk, list(range(hands))))
        send_chunk(chunk, False)
        return carry

    for chunk in range(early, chunks):
        compare(chunk, strips)
    for chunk in range(chunks):
        settle(ratio.at[pl.ds(0, hands - 1), pl.ds(0, 8 * both)], ratio_r.at[chunk])
    settle(reach.at[pl.ds(0, hands - 1)], reach_r)
    lax.fori_loop(0, chunks - 1, one_chunk, 0)
    finish(chunks - 1, partial(chunks - 1, list(range(hands))))
    send_chunk(chunks - 1, True)
    for chunk in range(chunks - 1):
        relay_chunk(chunk)
    settle(ratio.at[pl.ds(0, hands - 1)], ratio_s)
    settle(reach.at[pl.ds(0, hands - 1)], reach_s)
    settle(br_all.at[pl.ds(0, hands - 1)], br_s)

    settle(anc_all.at[pl.ds(0, leafs - 1)], anc_r)
    settle(anc_all.at[pl.ds(0, leafs - 1)], anc_s)
    lines_dev = levels * nodes_dev
    block = hands * 8
    together = max(width // block, 1)
    groups = [list(range(k, min(k + together, leafs))) for k in range(0, leafs, together)]

    def add_group(chunk, group, sums):
        own = pl.ds(group[0] * hands, len(group) * hands)
        tall = len(group) * block
        lines = [anc_all[source][:, chunk * block : (chunk + 1) * block] for source in group]
        lines = jnp.concatenate(lines, axis=1)
        node_rows = leaf * nodes_dev + lax.broadcasted_iota(jnp.int32, (nodes_dev, tall), 0)
        node_rows = node_rows.astype(F32)
        rows = [
            jnp.sum(units_all[chunk, source * hands : (source + 1) * hands], axis=0) for source in group
        ]
        unit = jnp.concatenate([row[:, 0:block] for row in rows], axis=1)
        part = values_all[chunk, own].astype(jnp.int32).astype(F32).reshape(tall, width)
        coarse = part.astype(BF16)
        fine = (part - coarse.astype(F32)).astype(BF16)
        pick = [jnp.where(lines[k : k + 1, :] == node_rows, unit, 0.0) for k in range(levels)]
        pick = jnp.concatenate(pick + [jnp.broadcast_to(unit, (8, tall))], axis=0).astype(BF16)
        sums = sums + jnp.dot(pick, coarse, preferred_element_type=F32)
        share = sum(row[:, block : block + 1] for row in rows)
        return sums + jnp.dot(pick, fine, preferred_element_type=F32), share

    sums = jnp.zeros((lines_dev + 8, width), F32)
    whole = jnp.zeros((1, 1), F32)
    for chunk in range(chunks):
        if chunk < chunks - 1:
            collect(chunk, peers - 1 - 2 * behind, 0)
            collect(chunk, behind, 2)
        else:
            collect(chunk, peers - 1, 0)
        for group in groups:
            sums, share = add_group(chunk, group, sums)
            whole = whole + share
    flat_out[0:lines_dev] = sums[0:lines_dev]
    for chunk in range(chunks):
        settle(values_all.at[chunk, pl.ds(0, peers - 1)], value_s)
        settle(units_all.at[chunk, pl.ds(0, peers - 1)], unit_s)
    best = whole / nodes / jnp.sum(br_row, axis=1, keepdims=True)
    line = lax.broadcasted_iota(jnp.int32, (8, width), 0)
    flat_out[lines_dev:] = jnp.where(line == 0, sums[lines_dev:] / nodes, best)


def spread_kernel(flat_ref, level_out, root_out, best_out):
    levels, nodes_dev, _ = level_out.shape
    for k in range(levels):
        level_out[k] = flat_ref[k * nodes_dev : (k + 1) * nodes_dev]
    root_out[...] = flat_ref[levels * nodes_dev]
    best_out[0, 0] = flat_ref[levels * nodes_dev + 1, 0]


def evaluate(
    upper, parents, roots, boards, opp_range, br_range, cards, opp_actions, kinds, stakes,
    br_actions, ranks, weights, leafs, hands, actions,
):
    levels, nodes_dev, width = upper.shape
    boards_dev, span, _ = weights.shape
    count = boards_dev // hands
    chunks = count // 8
    both = 2 * actions
    all_hands = ranks.shape[1]
    lanes = -(-boards_dev // 128) * 128
    dma = pltpu.SemaphoreType.DMA
    flat = pl.pallas_call(
        functools.partial(kernel, leafs, hands, levels, actions),
        out_shape=jax.ShapeDtypeStruct((levels * nodes_dev + 8, width), F32),
        in_specs=[vmem()] * 10 + [pl.BlockSpec(memory_space=pltpu.SMEM), hbm(), hbm()],
        out_specs=vmem(),
        scratch_shapes=[
            pltpu.VMEM((leafs, levels, nodes_dev, width), BF16),
            pltpu.VMEM((hands, count, span, width), BF16),
            pltpu.VMEM((count, all_hands), jnp.int32),
            pltpu.VMEM((hands, count * both, width), BF16),
            pltpu.VMEM((hands, count * both, width), BF16),
            pltpu.VMEM((hands, chunks, 8, width), BF16),
            pltpu.VMEM((hands, chunks, 8, width), BF16),
            pltpu.VMEM((8, lanes), F32),
            pltpu.VMEM((leafs, 8, lanes), F32),
            pltpu.VMEM((hands, 1, width), F32),
            pltpu.VMEM((8, lanes), F32),
            pltpu.VMEM((lanes, 8), F32),
            pltpu.VMEM((span, lanes), F32),
            pltpu.VMEM((lanes, span), F32),
            pltpu.VMEM((all_hands, all_hands), BF16),
            pltpu.VMEM((all_hands, all_hands), BF16),
            pltpu.VMEM((all_hands, all_hands), F8),
            pltpu.VMEM((count, all_hands, all_hands), F8),
            pltpu.VMEM((count, all_hands), F32),
            pltpu.VMEM((chunks, hands, 8, width), jnp.int16),
            pltpu.VMEM((chunks, leafs * hands, 8, width), jnp.int16),
            pltpu.VMEM((chunks, 1, 128), F32),
            pltpu.VMEM((chunks, leafs * hands, 1, 128), F32),
            dma(()), dma((max(leafs // 2, 1),)), dma(()), dma(()), dma(()),
            dma(()), dma((chunks,)), dma(()), dma(()), dma(()), dma(()),
            dma(()), dma((3, chunks)), dma(()), dma((3, chunks)),
            dma((chunks,)), dma((2,)),
        ],
        compiler_params=pltpu.CompilerParams(
            collective_id=0, has_side_effects=True, vmem_limit_bytes=VMEM_LIMIT
        ),
        name="evaluate",
    )(
        upper, parents, roots, boards, opp_range, br_range, cards, opp_actions, kinds, stakes,
        br_actions, ranks, weights,
    )
    return pl.pallas_call(
        spread_kernel,
        out_shape=(
            jax.ShapeDtypeStruct((levels, nodes_dev, width), F32),
            jax.ShapeDtypeStruct((width,), F32),
            jax.ShapeDtypeStruct((1, 1), F32),
        ),
        in_specs=[vmem()],
        out_specs=(vmem(), vmem(), pl.BlockSpec(memory_space=pltpu.SMEM)),
        name="spread",
    )(flat)


def local(
    opp_range,
    br_range,
    up_weight,
    up_parent,
    board_cards,
    hand_rank,
    root_parent,
    br_actions,
    opp_actions,
    leaf_kind,
    leaf_stake,
    opp_weight,
):
    hands_dev = up_weight.shape[2]
    boards_dev, hands_all = hand_rank.shape
    actions = opp_actions.shape[1]
    span = actions * actions
    leafs = lax.axis_size("leaf")
    hands = lax.axis_size("hand")
    cards = jnp.asarray(hand_cards(hands_all))
    boards = board_cards.T
    level_values, root, best = evaluate(
        up_weight,
        up_parent,
        root_parent[None, :],
        boards,
        opp_range[None, :],
        br_range[None, :],
        cards,
        opp_actions.T,
        leaf_kind.transpose(1, 2, 0).reshape(span, boards_dev),
        leaf_stake.transpose(1, 2, 0).reshape(span, boards_dev),
        br_actions,
        hand_rank,
        opp_weight.reshape(boards_dev, span, hands_dev),
        leafs,
        hands,
        actions,
    )
    return (level_values, root, best[0, 0])


def solution(mesh):
    in_specs = (
        P("hand"),
        P("hand"),
        P(None, "leaf", "hand"),
        P(),
        P("leaf", None),
        P("leaf", None),
        P("leaf"),
        P("leaf"),
        P("leaf", None),
        P("leaf", None, None),
        P("leaf", None, None),
        P("leaf", None, None, "hand"),
    )
    out_specs = (P(None, "leaf", "hand"), P("hand"), P())
    return jax.shard_map(local, mesh=mesh, in_specs=in_specs, out_specs=out_specs, check_vma=False)
```
